512 devices in a mesh: row: 16 (over z), col: 4 (over x), depth: 8 (over y, core).
Axes of the slice: x: 4, y: 4, z: 16, core: 2. Of those that a mesh axis runs over, the one named last changes fastest.
Arguments:
- tokens: bfloat16 [1024, 4608], P(('row', 'depth'), 'col'), may hold values from -6 to 6
- grad_out: bfloat16 [1024, 4608], P(('row', 'depth'), 'col'), may hold values from -6 to 6
- w_gate: bfloat16 [18432, 4608], P(('row', 'depth'), 'col'), may hold values from -0.09375 to 0.09375
- w_up: bfloat16 [18432, 4608], P(('row', 'depth'), 'col'), may hold values from -0.09375 to 0.09375
- w_down: bfloat16 [18432, 4608], P(('row', 'depth'), 'col'), may hold values from -0.046875 to 0.046875
Outputs:
- grad_in: bfloat16 [1024, 4608], P(('row', 'depth'), 'col')
- grad_gate_w: float32 [18432, 4608], P(('row', 'depth'), 'col')
- grad_up_w: float32 [18432, 4608], P(('row', 'depth'), 'col')
- grad_down_w: float32 [18432, 4608], P(('row', 'depth'), 'col')
- grad_rms: float32 [3], replicated
The draws below stay inside these ranges and needn't reach their ends.
All inputs are finite; a program needn't handle non-finite values.
Results may differ from the reference program's by a relative error of at most 0.0049.
Values may be sent and summed in bfloat16 or wider, within the bound.
A program may use at most 64 MiB of HBM per device.

```python
import jax
import jax.numpy as jnp
from jax import lax

D = 4608
FF = 18432
TOKENS = 1024


def shard_levels(key, shape, pieces, low, high):
    def one(position, blocks):
        steps = jax.random.uniform(jax.random.fold_in(jax.random.fold_in(key, 6), position), (blocks,), jnp.float32, low / len(pieces), high / len(pieces))
        return jnp.repeat(jnp.exp(steps), shape[position] // blocks).reshape((-1,) + (1,) * (len(shape) - position - 1))

    factor_of = one(*pieces[0])
    for cut in pieces[1:]:
        factor_of = factor_of * one(*cut)
    return factor_of


def centred(stream_key, extent, spread, most, cuts=(), kind=jnp.bfloat16):
    loudness = shard_levels(stream_key, extent, cuts, -0.22, 0.18) if cuts else 1.0
    drawn = jax.random.normal(stream_key, extent, jnp.float32) * spread * loudness
    return jnp.minimum(jnp.maximum(drawn, -most), most).astype(kind)


def setup_inputs(seed: int = 0) -> dict:
    seeds = jax.random.split(jax.random.key(seed), 6)
    return {
        "tokens": centred(seeds[0], (TOKENS, D), 1.0, 6.0, ((0, 128), (1, 4))),
        "grad_out": centred(seeds[1], (TOKENS, D), 1.0, 6.0, ((0, 128), (1, 4))),
        "w_gate": centred(seeds[2], (FF, D), D ** -0.5, 0.09375, ((0, 128), (1, 4))),
        "w_up": centred(seeds[3], (FF, D), D ** -0.5, 0.09375, ((0, 128), (1, 4))),
        "w_down": centred(seeds[4], (FF, D), FF ** -0.5, 0.046875, ((0, 128), (1, 4))),
    }


tanh_scale = 0.7978845608028654
cubic_coeff = 0.044715

def gelu_parts(pre_act):
    inner_arg = tanh_scale * (pre_act + cubic_coeff * pre_act * pre_act * pre_act)
    tanh_value = jnp.tanh(inner_arg)
    gelu_value = 0.5 * pre_act * (1.0 + tanh_value)
    gelu_slope = 0.5 * (1.0 + tanh_value) + 0.5 * pre_act * (1.0 - tanh_value * tanh_value) * tanh_scale * (1.0 + 3.0 * cubic_coeff * pre_act * pre_act)
    return (gelu_value, gelu_slope)

def dot_transposed(left_side, right_side):
    return lax.dot_general(left_side, right_side, (((1,), (1,)), ((), ())), preferred_element_type=jnp.float32)

def sum_over_rows(left_side, right_side):
    return lax.dot_general(left_side, right_side, (((0,), (0,)), ((), ())), preferred_element_type=jnp.float32)

def reference(tokens, grad_out, w_gate, w_up, w_down):
    gate_pre = dot_transposed(tokens, w_gate)
    up_pre = dot_transposed(tokens, w_up)
    grad_hidden = dot_transposed(grad_out, w_down)
    gelu_value, gelu_slope = gelu_parts(gate_pre)
    hidden = (gelu_value * up_pre).astype(jnp.bfloat16)
    grad_gate = (grad_hidden * up_pre * gelu_slope).astype(jnp.bfloat16)
    grad_up = (grad_hidden * gelu_value).astype(jnp.bfloat16)
    grad_in = (jnp.dot(grad_gate, w_gate, preferred_element_type=jnp.float32) + jnp.dot(grad_up, w_up, preferred_element_type=jnp.float32)).astype(jnp.bfloat16)
    grad_gate_w = sum_over_rows(grad_gate, tokens)
    grad_up_w = sum_over_rows(grad_up, tokens)
    grad_down_w = sum_over_rows(hidden, grad_out)
    entries = jnp.float32(D * FF)
    grad_rms = jnp.stack([jnp.sqrt(jnp.sum(grad_gate_w * grad_gate_w) / entries), jnp.sqrt(jnp.sum(grad_up_w * grad_up_w) / entries), jnp.sqrt(jnp.sum(grad_down_w * grad_down_w) / entries)])
    return (grad_in, grad_gate_w, grad_up_w, grad_down_w, grad_rms)
```

```python
import functools

import jax
import jax.numpy as jnp
from jax import lax
from jax.experimental import pallas as pl
from jax.experimental.pallas import tpu as pltpu
from jax.sharding import Mesh
from jax.sharding import PartitionSpec as P

D = 4608
FF = 18432
ROW_DEPTH = ("row", "depth_0", "depth_1")
Z, X, Y = 16, 4, 4
STEPS = Z // 2
F32 = jnp.float32
BF16 = jnp.bfloat16
MESH = pl.DeviceIdType.MESH

tanh_scale = 0.7978845608028654
cubic_coeff = 0.044715


def gelu_parts(pre_act):
    inner_arg = tanh_scale * (pre_act + cubic_coeff * pre_act * pre_act * pre_act)
    tanh_value = jnp.tanh(inner_arg)
    gelu_value = 0.5 * pre_act * (1.0 + tanh_value)
    gelu_slope = 0.5 * (1.0 + tanh_value) + 0.5 * pre_act * (
        1.0 - tanh_value * tanh_value
    ) * tanh_scale * (1.0 + 3.0 * cubic_coeff * pre_act * pre_act)
    return (gelu_value, gelu_slope)


def geglu_backward(gate_pre, up_pre, grad_hidden):
    gelu_value, gelu_slope = gelu_parts(gate_pre)
    return (
        gelu_value * up_pre,
        grad_hidden * up_pre * gelu_slope,
        grad_hidden * gelu_value,
    )


def nt(a, b):
    return lax.dot_general(a, b, (((1,), (1,)), ((), ())), preferred_element_type=F32)


def nn(a, b):
    return lax.dot_general(a, b, (((1,), (0,)), ((), ())), preferred_element_type=F32)


def tn(a, b):
    return lax.dot_general(a, b, (((0,), (0,)), ((), ())), preferred_element_type=F32)


def kernel(
    x_ref, dy_ref, wg_ref, wu_ref, wd_ref,
    gi_out, gw_out, uw_out, dw_out, rms_out,
    blk, wm, wlx, wld, pf, sx, rx, g, xs, gi, sy, ry, sz, rz, acc,
    wo, wp, wr, rb, sb,
    ysend, yrecv, wlocal, wsend, wrecv, fsend, frecv,
    xsend, xrecv, gsend, grecv, rysend, ryrecv, rzsend, rzrecv,
    psend, precv, osend, nsend, nrecv,
):
    z = lax.axis_index("row")
    x = lax.axis_index("col")
    y = lax.axis_index("depth_0")
    k = lax.axis_index("depth_1")
    other = 1 - k

    def zdev(o):
        return {"row": lax.rem(z + o, Z)}

    def xdev(o):
        return {"col": lax.rem(x + o, X)}

    def ydev(o):
        return {"depth_0": lax.rem(y + o, Y)}

    mate = {"depth_1": other}

    def rcopy(src, dst, s, r, dev):
        return pltpu.make_async_remote_copy(
            src_ref=src, dst_ref=dst, send_sem=s, recv_sem=r, device_id=dev, device_id_type=MESH
        )

    def wait_bytes(ref, sem):
        pltpu.make_async_copy(ref, ref, sem).wait()

    barrier = pltpu.get_barrier_semaphore()
    for o in range(1, Z):
        pl.semaphore_signal(barrier, inc=1, device_id=zdev(o), device_id_type=MESH)
    for o in range(1, X):
        pl.semaphore_signal(barrier, inc=1, device_id=xdev(o), device_id_type=MESH)
    for o in range(1, Y):
        pl.semaphore_signal(barrier, inc=1, device_id=ydev(o), device_id_type=MESH)
    pl.semaphore_signal(barrier, inc=1, device_id=mate, device_id_type=MESH)

    weights = (wg_ref, wu_ref, wd_ref)

    def tail_of(p):
        return (wlx, 0) if p == 0 else (wlx, 32) if p == 1 else (wld, 64)

    wlx[64:128, :] = jnp.zeros((64, wlx.shape[1]), BF16)
    wld[0:64, :] = jnp.zeros((64, wld.shape[1]), BF16)
    wld[96:128, :] = jnp.zeros((32, wld.shape[1]), BF16)
    local = []
    for p in range(3):
        tail, at = tail_of(p)
        local.append(
            pltpu.make_async_copy(weights[p].at[0:128], wm.at[p, 0:128], wlocal.at[2 * p])
        )
        local.append(
            pltpu.make_async_copy(
                weights[p].at[128:144], tail.at[at : at + 16], wlocal.at[2 * p + 1]
            )
        )
    for c in local:
        c.start()
    blk[0, 0, 0, pl.ds(y, 1)] = x_ref[...][None]
    blk[0, 0, 1, pl.ds(y, 1)] = dy_ref[...][None]

    pl.semaphore_wait(barrier, (Z - 1) + (X - 1) + (Y - 1) + 1)

    ycopies = []
    for xd, src in ((0, x_ref), (1, dy_ref)):
        for o in (1, 3, 2):
            c = rcopy(
                src, blk.at[0, 0, xd, y], ysend.at[xd, o - 1], yrecv.at[xd, o - 1], ydev(o)
            )
            c.start()
            ycopies.append(c)
    wcopies = []
    for p in range(3):
        tail, at = tail_of(p)
        wcopies.append(
            rcopy(
                weights[p].at[0:128], wm.at[p, 128:256], wsend.at[2 * p], wrecv.at[2 * p], mate
            )
        )
        wcopies.append(
            rcopy(
                weights[p].at[128:144],
                tail.at[at + 16 : at + 32],
                wsend.at[2 * p + 1],
                wrecv.at[2 * p + 1],
                mate,
            )
        )
    for c in wcopies:
        c.start()

    def ring(direction, src_dir, src_slot, dst_dir, dst_slot, xd, sem_slot):
        return rcopy(
            blk.at[src_dir, src_slot, xd],
            blk.at[dst_dir, dst_slot, xd],
            fsend.at[direction, sem_slot, xd],
            frecv.at[dst_dir, dst_slot, xd],
            zdev(1) if direction == 0 else zdev(Z - 1),
        )

    for xd in range(2):
        for o in range(1, Y):
            ycopies[3 * xd + o - 1].wait_recv()
        ring(0, 0, 0, 0, 1, xd, 0).start()
        ring(1, 0, 0, 1, 1, xd, 0).start()

    for c in local:
        c.wait()
    for c in wcopies:
        c.wait_recv()

    def got(direction, slot, xd):
        wait_bytes(blk.at[direction, slot, xd], frecv.at[direction, slot, xd])

    def stage_a(t):
        @pl.when(t < STEPS)
        def _():
            for xd in range(2):
                for direction in range(2):
                    got(direction, t, xd)

                    @pl.when(t < STEPS - 1)
                    def _():
                        ring(direction, direction, t, direction, t + 1, xd, t).start()

                    if direction == xd:

                        @pl.when(t == STEPS - 1)
                        def _():
                            ring(direction, direction, t, 1, 0, xd, t).start()

        @pl.when(t == STEPS)
        def _():
            got(1, 0, 0)
            got(1, 0, 1)

        slot = lax.rem(t, STEPS)
        it = t - 1
        xv = blk[:, pl.ds(slot, 1), 0].astype(F32).reshape(64, -1).astype(BF16)
        dv = blk[:, pl.ds(slot, 1), 1].astype(F32).reshape(64, -1).astype(BF16)
        xs[0, pl.ds(it, 1)] = xv[None]
        xs[1, pl.ds(it, 1)] = dv[None]
        parts = (
            (nt(xv, wm[0]), 0),
            (nt(xv, wm[1]), 256),
            (nt(dv, wm[2]), 512),
            (nt(xv, wlx[...]) + nt(dv, wld[...]), 768),
        )
        for value, at in parts:
            pf[pl.ds(it, 1), :, :, at : at + value.shape[1]] = value.reshape(1, X, 16, -1)
        for o in (2, 1, 3):
            j = lax.rem(x + o, X)
            sx[it, o - 1] = pf[it, j].astype(BF16)
            rcopy(
                sx.at[it, o - 1], rx.at[it, o - 1], xsend.at[it], xrecv.at[it], xdev(o)
            ).start()

    lane = lax.broadcasted_iota(jnp.int32, (16, 128), 1)

    def stage_b(i):
        wait_bytes(rx.at[i], xrecv.at[i])
        total = pf[i, x]
        for o in range(3):
            total = total + rx[i, o].astype(F32)
        hid, gg, gu = geglu_backward(total[:, 0:256], total[:, 256:512], total[:, 512:768])
        left = total[:, 768:896]
        hid_l, gg_l, gu_l = geglu_backward(
            left, pltpu.roll(left, 96, 1), pltpu.roll(left, 64, 1)
        )
        packed = jnp.where(
            lane < 32,
            gg_l,
            jnp.where(
                lane < 64,
                pltpu.roll(gu_l, 32, 1),
                jnp.where(lane < 96, pltpu.roll(hid_l, 64, 1), 0.0),
            ),
        )
        g[i, x, :, 0:256] = gg.astype(BF16)
        g[i, x, :, 256:512] = gu.astype(BF16)
        g[i, x, :, 512:768] = hid.astype(BF16)
        g[i, x, :, 768:896] = packed.astype(BF16)
        for o in (2, 1, 3):
            rcopy(g.at[i, x], g.at[i, x], gsend.at[i], grecv.at[i], xdev(o)).start()

    def stage_c(i):
        wait_bytes(g.at[i, 0:3], grecv.at[i])
        gv = g[i].reshape(64, 896)
        part = (
            nn(gv[:, 0:256], wm[0]) + nn(gv[:, 256:512], wm[1]) + nn(gv[:, 768:896], wlx[...])
        )
        gi[pl.ds(i, 1)] = part.reshape(1, 2, Y, 8, -1)
        for o in (2, 1, 3):
            j = lax.rem(y + o, Y)
            sy[i, o - 1] = gi[i, :, j].astype(BF16)
            rcopy(
                sy.at[i, o - 1], ry.at[i, o - 1], rysend.at[i], ryrecv.at[i], ydev(o)
            ).start()

    def stage_d(i):
        wait_bytes(ry.at[i], ryrecv.at[i])
        total = gi[i, :, y]
        for o in range(3):
            total = total + ry[i, o].astype(F32)
        sz[i] = total.astype(BF16)
        t = i + 1

        @pl.when(t < STEPS)
        def _():
            rcopy(
                sz.at[i, 0], rz.at[t - 1], rzsend.at[i, 0], rzrecv, zdev(Z - t)
            ).start()

        @pl.when(t == STEPS)
        def _():
            acc[...] = total[0]

        rcopy(
            sz.at[i, 1], rz.at[STEPS - 2 + t], rzsend.at[i, 1], rzrecv, zdev(t)
        ).start()

    def step(t, carry):
        pl.when(t <= STEPS)(lambda: stage_a(t))
        pl.when((t >= 2) & (t <= STEPS + 1))(lambda: stage_b(t - 2))
        pl.when((t >= 3) & (t <= STEPS + 2))(lambda: stage_c(t - 3))
        pl.when(t >= 4)(lambda: stage_d(t - 4))
        return carry

    lax.fori_loop(1, STEPS + 3, step, 0)

    tokens = STEPS * 64
    gall = g[...].reshape(tokens, 896)
    xall = xs[0].reshape(tokens, -1)
    dall = xs[1].reshape(tokens, -1)
    tail_x = tn(gall[:, 768:896], xall)
    tail_d = tn(gall[:, 768:896], dall)
    tails = (tail_x[0:32], tail_x[32:64], tail_d[64:96])
    pcopies = []
    for p, right in ((0, xall), (1, xall), (2, dall)):
        main = tn(gall[:, 256 * p : 256 * p + 256], right)
        wp[p, 0:128] = main[128:256]
        wp[p, 128:144] = tails[p][16:32]
        c = rcopy(wp.at[p], wr.at[p], psend.at[p], precv.at[p], mate)
        c.start()
        pcopies.append(c)
        wo[p, 0:128] = main[0:128]
        wo[p, 128:144] = tails[p][0:16]

    stage_d(STEPS - 1)

    outs = (gw_out, uw_out, dw_out)
    ocopies = []
    squares = []
    for p in range(3):
        pcopies[p].wait_recv()
        total = wo[p] + wr[p]
        wo[p] = total
        c = pltpu.make_async_copy(wo.at[p], outs[p], osend.at[p])
        c.start()
        ocopies.append(c)
        squares.append(jnp.sum((total * total).reshape(18, 8, -1), axis=0))
    lanes = lax.broadcasted_iota(jnp.int32, (8, 128), 1)
    value = jnp.zeros((8, 128), F32)
    for p in range(3):
        value = jnp.where(lanes == p, jnp.sum(squares[p]), value)

    ncopies = []

    def norm_stage(stage, value, count, me, dev):
        sb[stage] = value
        rb[stage, me] = value
        for o in range(1, count):
            rcopy(
                sb.at[stage], rb.at[stage, me], nsend.at[stage], nrecv.at[stage], dev(o)
            ).start()
        wait_bytes(rb.at[stage, 0 : count - 1], nrecv.at[stage])
        total = rb[stage, 0]
        for j in range(1, count):
            total = total + rb[stage, j]
        return total

    value = norm_stage(0, value, 2, k, lambda o: mate)
    value = norm_stage(1, value, X, x, xdev)
    value = norm_stage(2, value, Y, y, ydev)
    value = norm_stage(3, value, Z, z, zdev)
    rms_out[...] = jnp.sqrt(value / F32(D * FF))

    wait_bytes(rz, rzrecv)
    total = acc[...]
    for j in range(Z - 1):
        total = total + rz[j].astype(F32)
    gi_out[...] = total.astype(BF16)

    for c in ycopies:
        c.wait_send()
    for c in wcopies:
        c.wait_send()
    for s in range(STEPS):
        for xd in range(2):
            for direction in range(2):
                if s < STEPS - 1 or direction == xd:
                    wait_bytes(blk.at[direction, 0, xd], fsend.at[direction, s, xd])
        wait_bytes(sx.at[s], xsend.at[s])
        wait_bytes(g.at[s, 0:3], gsend.at[s])
        wait_bytes(sy.at[s], rysend.at[s])
        if s < STEPS - 1:
            wait_bytes(sz.at[s, 0], rzsend.at[s, 0])
        wait_bytes(sz.at[s, 1], rzsend.at[s, 1])
    for c in pcopies:
        c.wait_send()
    for c in ocopies:
        c.wait()
    for stage, count in enumerate((2, X, Y, Z)):
        wait_bytes(rb.at[stage, 0 : count - 1], nsend.at[stage])


def body(tokens, grad_out, w_gate, w_up, w_down):
    c = tokens.shape[1]
    h = w_gate.shape[0]
    vmem = pl.BlockSpec(memory_space=pltpu.VMEM)
    hbm = pl.BlockSpec(memory_space=pl.ANY)
    dma = pltpu.SemaphoreType.DMA
    wgrad = jax.ShapeDtypeStruct((h, c), F32)
    grad_in, gw, uw, dw, rms = pl.pallas_call(
        kernel,
        out_shape=(
            jax.ShapeDtypeStruct(tokens.shape, BF16),
            wgrad,
            wgrad,
            wgrad,
            jax.ShapeDtypeStruct((8, 128), F32),
        ),
        in_specs=[vmem, vmem, hbm, hbm, hbm],
        out_specs=(vmem, hbm, hbm, hbm, vmem),
        scratch_shapes=[
            pltpu.VMEM((2, STEPS, 2, Y, 8, c), BF16),
            pltpu.VMEM((3, 256, c), BF16),
            pltpu.VMEM((128, c), BF16),
            pltpu.VMEM((128, c), BF16),
            pltpu.VMEM((STEPS, X, 16, 896), F32),
            pltpu.VMEM((STEPS, 3, 16, 896), BF16),
            pltpu.VMEM((STEPS, 3, 16, 896), BF16),
            pltpu.VMEM((STEPS, X, 16, 896), BF16),
            pltpu.VMEM((2, STEPS, 64, c), BF16),
            pltpu.VMEM((STEPS, 2, Y, 8, c), F32),
            pltpu.VMEM((STEPS, 3, 2, 8, c), BF16),
            pltpu.VMEM((STEPS, 3, 2, 8, c), BF16),
            pltpu.VMEM((STEPS, 2, 8, c), BF16),
            pltpu.VMEM((Z - 1, 8, c), BF16),
            pltpu.VMEM((8, c), F32),
            pltpu.VMEM((3, h, c), F32),
            pltpu.VMEM((3, h, c), F32),
            pltpu.VMEM((3, h, c), F32),
            pltpu.VMEM((4, Z, 8, 128), F32),
            pltpu.VMEM((4, 8, 128), F32),
            dma((2, 3)), dma((2, 3)), dma((6,)), dma((6,)), dma((6,)),
            dma((2, STEPS, 2)), dma((2, STEPS, 2)),
            dma((STEPS,)), dma((STEPS,)), dma((STEPS,)), dma((STEPS,)),
            dma((STEPS,)), dma((STEPS,)), dma((STEPS, 2)), dma,
            dma((3,)), dma((3,)), dma((3,)), dma((4,)), dma((4,)),
        ],
        compiler_params=pltpu.CompilerParams(
            collective_id=0, has_side_effects=True, vmem_limit_bytes=60 * 1024 * 1024
        ),
    )(tokens, grad_out, w_gate, w_up, w_down)
    return (grad_in, gw, uw, dw, rms[0, 0:3])


def solution(mesh):
    torus = Mesh(
        mesh.devices.reshape(mesh.shape["row"], mesh.shape["col"], 4, 2),
        ("row", "col", "depth_0", "depth_1"),
    )
    placed = P(ROW_DEPTH, "col")
    return jax.shard_map(
        body,
        mesh=torus,
        in_specs=(placed,) * 5,
        out_specs=(placed, placed, placed, placed, P()),
        check_vma=False,
    )
```

```python
import functools

import jax
import jax.numpy as jnp
from jax import lax
from jax.experimental import pallas as pl
from jax.experimental.pallas import tpu as pltpu
from jax.sharding import Mesh
from jax.sharding import PartitionSpec as P

D = 4608
FF = 18432
ROW_DEPTH = ("row", "depth_0", "depth_1")
Z, X, Y = 16, 4, 4
STEPS = Z // 2
F32 = jnp.float32
BF16 = jnp.bfloat16
MESH = pl.DeviceIdType.MESH

tanh_scale = 0.7978845608028654
cubic_coeff = 0.044715


def gelu_parts(pre_act):
    inner_arg = tanh_scale * (pre_act + cubic_coeff * pre_act * pre_act * pre_act)
    tanh_value = jnp.tanh(inner_arg)
    gelu_value = 0.5 * pre_act * (1.0 + tanh_value)
    gelu_slope = 0.5 * (1.0 + tanh_value) + 0.5 * pre_act * (
        1.0 - tanh_value * tanh_value
    ) * tanh_scale * (1.0 + 3.0 * cubic_coeff * pre_act * pre_act)
    return (gelu_value, gelu_slope)


def geglu_backward(gate_pre, up_pre, grad_hidden):
    gelu_value, gelu_slope = gelu_parts(gate_pre)
    return (
        gelu_value * up_pre,
        grad_hidden * up_pre * gelu_slope,
        grad_hidden * gelu_value,
    )


def nt(a, b):
    return lax.dot_general(a, b, (((1,), (1,)), ((), ())), preferred_element_type=F32)


def nn(a, b):
    return lax.dot_general(a, b, (((1,), (0,)), ((), ())), preferred_element_type=F32)


def tn(a, b):
    return lax.dot_general(a, b, (((0,), (0,)), ((), ())), preferred_element_type=F32)


def kernel(
    x_ref, dy_ref, wg_ref, wu_ref, wd_ref,
    gi_out, w_out, rms_out,
    blk, wm, wlx, wld, pf, sx, rx, g, xs, mxs, mg, gi, sy, ry, sz, rz, acc,
    plane, line, sb,
    ysend, yrecv, wlocal, wsend, wrecv, fsend, frecv,
    xsend, xrecv, gsend, grecv, rysend, ryrecv, rzsend, rzrecv,
    mxsend, mxrecv, mgsend, mgrecv, nsend, nrecv,
):
    z = lax.axis_index("row")
    x = lax.axis_index("col")
    y = lax.axis_index("depth_0")
    k = lax.axis_index("depth_1")

    def zdev(o):
        return {"row": lax.rem(z + o, Z)}

    def xdev(o):
        return {"col": lax.rem(x + o, X)}

    def ydev(o):
        return {"depth_0": lax.rem(y + o, Y)}

    mate = {"depth_1": 1 - k}

    def rcopy(src, dst, s, r, dev):
        return pltpu.make_async_remote_copy(
            src_ref=src, dst_ref=dst, send_sem=s, recv_sem=r, device_id=dev, device_id_type=MESH
        )

    def wait_bytes(ref, sem, name="w"):
        with jax.named_scope("wait_" + name):
            pltpu.make_async_copy(ref, ref, sem).wait()

    barrier = pltpu.get_barrier_semaphore()
    near = [zdev(1), zdev(Z - 1), mate]
    near += [xdev(o) for o in range(1, X)] + [ydev(o) for o in range(1, Y)]
    for dev in near:
        pl.semaphore_signal(barrier, inc=1, device_id=dev, device_id_type=MESH)

    weights = (wg_ref, wu_ref, wd_ref)

    def tail_of(p):
        return (wlx, 0) if p == 0 else (wlx, 32) if p == 1 else (wld, 64)

    local = []
    for p in range(3):
        tail, at = tail_of(p)
        local.append(
            pltpu.make_async_copy(weights[p].at[0:128], wm.at[p, 0:128], wlocal.at[2 * p])
        )
        local.append(
            pltpu.make_async_copy(
                weights[p].at[128:144], tail.at[at : at + 16], wlocal.at[2 * p + 1]
            )
        )
    for c in local:
        c.start()
    wlx[64:128, :] = jnp.zeros((64, wlx.shape[1]), BF16)
    wld[0:64, :] = jnp.zeros((64, wld.shape[1]), BF16)
    wld[96:128, :] = jnp.zeros((32, wld.shape[1]), BF16)
    blk[0, 0, 0, pl.ds(y, 1)] = x_ref[...][None]
    blk[0, 0, 1, pl.ds(y, 1)] = dy_ref[...][None]

    with jax.named_scope("barrier"):
        pl.semaphore_wait(barrier, len(near))

    ycopies = []
    for xd, src in ((0, x_ref), (1, dy_ref)):
        for o in (2, 1, 3):
            c = rcopy(
                src, blk.at[0, 0, xd, y], ysend.at[xd, o - 1], yrecv.at[xd, o - 1], ydev(o)
            )
            c.start()
            ycopies.append(c)
    wcopies = []
    for p in range(3):
        tail, at = tail_of(p)
        wcopies.append(
            rcopy(
                weights[p].at[0:128], wm.at[p, 128:256], wsend.at[2 * p], wrecv.at[2 * p], mate
            )
        )
        wcopies.append(
            rcopy(
                weights[p].at[128:144],
                tail.at[at + 16 : at + 32],
                wsend.at[2 * p + 1],
                wrecv.at[2 * p + 1],
                mate,
            )
        )
    for c in wcopies:
        c.start()

    def quarter(direction, slot, q):
        half = 2 * (q % 2)
        return blk.at[direction, slot, q // 2, half : half + 2]

    def ring(direction, src_dir, src_slot, dst_dir, dst_slot, q):
        return rcopy(
            quarter(src_dir, src_slot, q),
            quarter(dst_dir, dst_slot, q),
            fsend.at[direction, src_slot, q],
            frecv.at[dst_dir, dst_slot, q],
            zdev(1) if direction == 0 else zdev(Z - 1),
        )

    for xd in range(2):
        with jax.named_scope("wait_y"):
            for o in range(3):
                ycopies[3 * xd + o].wait_recv()
        for q in (2 * xd, 2 * xd + 1):
            ring(0, 0, 0, 0, 1, q).start()
            ring(1, 0, 0, 1, 1, q).start()

    with jax.named_scope("wait_w"):
        for c in local:
            c.wait()
        for c in wcopies:
            c.wait_recv()

    def got(direction, slot, q):
        wait_bytes(quarter(direction, slot, q), frecv.at[direction, slot, q], "ring")

    def poll(t, q):
        @pl.when(t < STEPS)
        def _():
            for direction in range(2):
                got(direction, t, q)

                @pl.when(t < STEPS - 1)
                def _():
                    ring(direction, direction, t, direction, t + 1, q).start()

                if direction == q // 2:

                    @pl.when(t == STEPS - 1)
                    def _():
                        ring(direction, direction, t, 1, 0, q).start()

        @pl.when(t == STEPS)
        def _():
            got(1, 0, q)

    def rows_of(t, xd):
        slot = lax.rem(t, STEPS)
        return blk[:, pl.ds(slot, 1), xd].astype(F32).reshape(64, -1).astype(BF16)

    def put(i, value, at):
        pf[pl.ds(i, 1), :, :, at : at + value.shape[1]] = value.reshape(1, X, 16, -1)

    def to_mate(src, dst, s, r):
        rcopy(src, dst, s, r, mate).start()

    lane = lax.broadcasted_iota(jnp.int32, (16, 128), 1)

    def stage_b(i):
        wait_bytes(rx.at[i], xrecv.at[i], "rx")
        total = pf[i, x]
        for o in range(3):
            total = total + rx[i, o].astype(F32)
        hid, gg, gu = geglu_backward(total[:, 0:256], total[:, 256:512], total[:, 512:768])
        left = total[:, 768:896]
        hid_l, gg_l, gu_l = geglu_backward(
            left, pltpu.roll(left, 96, 1), pltpu.roll(left, 64, 1)
        )
        packed = jnp.where(
            lane < 32,
            gg_l,
            jnp.where(
                lane < 64,
                pltpu.roll(gu_l, 32, 1),
                jnp.where(lane < 96, pltpu.roll(hid_l, 64, 1), 0.0),
            ),
        )
        g[i, x, :, 0:256] = gg.astype(BF16)
        g[i, x, :, 256:512] = gu.astype(BF16)
        g[i, x, :, 512:768] = hid.astype(BF16)
        g[i, x, :, 768:896] = packed.astype(BF16)
        for o in (2, 1, 3):
            rcopy(g.at[i, x], g.at[i, x], gsend.at[i], grecv.at[i], xdev(o)).start()

    def stage_c(i):
        wait_bytes(g.at[i, 0:3], grecv.at[i], "g")
        to_mate(g.at[i], mg.at[i], mgsend.at[i], mgrecv.at[i])
        gv = g[i].reshape(64, 896)
        part = (
            nn(gv[:, 0:256], wm[0]) + nn(gv[:, 256:512], wm[1]) + nn(gv[:, 768:896], wlx[...])
        )
        gi[pl.ds(i, 1)] = part.reshape(1, 2, Y, 8, -1)
        for o in (2, 1, 3):
            j = lax.rem(y + o, Y)
            sy[i, o - 1] = gi[i, :, j].astype(BF16)
            rcopy(
                sy.at[i, o - 1], ry.at[i, o - 1], rysend.at[i], ryrecv.at[i], ydev(o)
            ).start()

    def stage_d(i):
        wait_bytes(ry.at[i], ryrecv.at[i], "ry")
        total = gi[i, :, y]
        for o in range(3):
            total = total + ry[i, o].astype(F32)
        sz[i] = total.astype(BF16)
        t = i + 1

        @pl.when(t < STEPS)
        def _():
            rcopy(
                sz.at[i, 0], rz.at[t - 1], rzsend.at[i, 0], rzrecv, zdev(Z - t)
            ).start()

        @pl.when(t == STEPS)
        def _():
            acc[...] = total[0]

        rcopy(
            sz.at[i, 1], rz.at[STEPS - 2 + t], rzsend.at[i, 1], rzrecv, zdev(t)
        ).start()

    def scoped(f, name):
        def inner(*args):
            with jax.named_scope("stage_" + name):
                f(*args)
        return inner

    stage_b, stage_c, stage_d = scoped(stage_b, "b"), scoped(stage_c, "c"), scoped(stage_d, "d")

    def step(t, carry):
        i = t - 1
        poll(t, 0)
        poll(t, 1)
        pl.when(t >= 3)(lambda: stage_b(t - 3))
        with jax.named_scope("a_x"):
            xv = rows_of(t, 0)
            xs[0, pl.ds(i, 1)] = xv[None]
            put(i, nt(xv, wm[0]), 0)
            put(i, nt(xv, wm[1]), 256)
            left = nt(xv, wlx[...])
        poll(t, 2)
        pl.when(t >= 5)(lambda: stage_c(t - 5))
        poll(t, 3)
        with jax.named_scope("a_d"):
            dv = rows_of(t, 1)
            xs[1, pl.ds(i, 1)] = dv[None]
            put(i, nt(dv, wm[2]), 512)
            put(i, left + nt(dv, wld[...]), 768)
            for o in (2, 1, 3):
                j = lax.rem(x + o, X)
                sx[i, o - 1] = pf[i, j].astype(BF16)
                rcopy(
                    sx.at[i, o - 1], rx.at[i, o - 1], xsend.at[i], xrecv.at[i], xdev(o)
                ).start()
            for xd in range(2):
                to_mate(xs.at[xd, i], mxs.at[xd, i], mxsend.at[xd, i], mxrecv.at[xd, i])
        pl.when(t >= 7)(lambda: stage_d(t - 7))
        return carry

    lax.fori_loop(1, STEPS + 1, step, 0)

    def own(lanes, first, last, source):
        count = 64 * (last - first)
        return source[first:last].reshape(count, 896)[:, lanes : lanes + 128]

    def wgrad_of(first, last, gsrc, xsrc):
        count = 64 * (last - first)
        xa = xsrc[0, first:last].reshape(count, -1)
        da = xsrc[1, first:last].reshape(count, -1)
        tail = own(768, first, last, gsrc)
        tail_x, tail_d = tn(tail, xa), tn(tail, da)
        return (
            (tn(own(0, first, last, gsrc), xa), tail_x, 0),
            (tn(own(256, first, last, gsrc), xa), tail_x, 32),
            (tn(own(512, first, last, gsrc), da), tail_d, 64),
        )

    def wgrad_mine(first, last, fresh):
        for p, (main, tail, at) in enumerate(wgrad_of(first, last, g, xs)):
            low = tail[at : at + 16]
            w_out[p, 0:128] = main if fresh else w_out[p, 0:128] + main
            w_out[p, 128:144] = low if fresh else w_out[p, 128:144] + low

    def mate_own(lanes, first, last):
        return own(lanes + 128, first, last, mg)

    def wgrad_mate(first, last):
        for i in range(first, last):
            wait_bytes(mg.at[i], mgrecv.at[i], "mg")
            for xd in range(2):
                wait_bytes(mxs.at[xd, i], mxrecv.at[xd, i], "mx")
        count = 64 * (last - first)
        xa = mxs[0, first:last].reshape(count, -1)
        da = mxs[1, first:last].reshape(count, -1)
        tail = own(768, first, last, mg)
        tail_x, tail_d = tn(tail, xa), tn(tail, da)
        for p, (right, tails, at) in enumerate(
            ((xa, tail_x, 16), (xa, tail_x, 48), (da, tail_d, 80))
        ):
            w_out[p, 0:128] = w_out[p, 0:128] + tn(mate_own(256 * p, first, last), right)
            w_out[p, 128:144] = w_out[p, 128:144] + tails[at : at + 16]

    half = STEPS // 2
    stage_b(STEPS - 2)
    stage_c(STEPS - 4)
    stage_d(STEPS - 6)
    with jax.named_scope("wgrad_1"):
        wgrad_mine(0, half, True)
        wgrad_mate(0, half)
    stage_b(STEPS - 1)
    stage_c(STEPS - 3)
    stage_d(STEPS - 5)
    stage_c(STEPS - 2)
    stage_d(STEPS - 4)
    with jax.named_scope("wgrad_2"):
        wgrad_mine(half, STEPS - 1, False)
        wgrad_mate(half, STEPS - 1)
    stage_c(STEPS - 1)
    stage_d(STEPS - 3)
    stage_d(STEPS - 2)
    with jax.named_scope("wgrad_3"):
        wgrad_mine(STEPS - 1, STEPS, False)
        wgrad_mate(STEPS - 1, STEPS)

    with jax.named_scope("squares"):
        lanes = lax.broadcasted_iota(jnp.int32, (8, 128), 1)
        value = jnp.zeros((8, 128), F32)
        for p in range(3):
            total = w_out[p]
            square = jnp.sum((total * total).reshape(18, 8, -1), axis=0)
            value = jnp.where(lanes == p, jnp.sum(square), value)

    here = (x * Y + y) * 2 + k
    sb[0] = value
    plane[here] = value
    for dx in (2, 1, 3, 0):
        for dy in (2, 1, 3, 0):
            for dk in (1, 0):
                if dx or dy or dk:
                    rcopy(
                        sb.at[0],
                        plane.at[here],
                        nsend.at[0],
                        nrecv.at[0],
                        {
                            "col": lax.rem(x + dx, X),
                            "depth_0": lax.rem(y + dy, Y),
                            "depth_1": lax.rem(k + dk, 2),
                        },
                    ).start()
    stage_d(STEPS - 1)
    others = X * Y * 2 - 1
    wait_bytes(plane.at[0:others], nrecv.at[0], "plane")
    value = jnp.sum(plane[...], axis=0)
    sb[1] = value
    line[z] = value
    for o in range(Z // 2, 0, -1):
        for d in sorted({o, Z - o}):
            rcopy(sb.at[1], line.at[z], nsend.at[1], nrecv.at[1], zdev(d)).start()

    wait_bytes(rz, rzrecv, "rz")
    total = acc[...]
    for j in range(Z - 1):
        total = total + rz[j].astype(F32)
    gi_out[...] = total.astype(BF16)

    for c in ycopies:
        c.wait_send()
    for c in wcopies:
        c.wait_send()
    for s in range(STEPS):
        for q in range(4):
            for direction in range(2):
                if s < STEPS - 1 or direction == q // 2:
                    wait_bytes(quarter(direction, 0, q), fsend.at[direction, s, q])
        wait_bytes(sx.at[s], xsend.at[s])
        wait_bytes(g.at[s, 0:3], gsend.at[s])
        wait_bytes(mg.at[s], mgsend.at[s])
        for xd in range(2):
            wait_bytes(mxs.at[xd, s], mxsend.at[xd, s])
        wait_bytes(sy.at[s], rysend.at[s])
        if s < STEPS - 1:
            wait_bytes(sz.at[s, 0], rzsend.at[s, 0])
        wait_bytes(sz.at[s, 1], rzsend.at[s, 1])
    wait_bytes(plane.at[0:others], nsend.at[0])

    wait_bytes(line.at[0 : Z - 1], nrecv.at[1], "line")
    rms_out[...] = jnp.sqrt(jnp.sum(line[...], axis=0) / F32(D * FF))
    wait_bytes(line.at[0 : Z - 1], nsend.at[1])


def finish(gi_ref, w_ref, rms_ref, gi_out, gw_out, uw_out, dw_out, rms_out, sems):
    copies = [
        pltpu.make_async_copy(w_ref.at[p], out, sems.at[p])
        for p, out in enumerate((gw_out, uw_out, dw_out))
    ]
    copies.append(pltpu.make_async_copy(gi_ref, gi_out, sems.at[3]))
    for c in copies:
        c.start()
    row = rms_ref[0:1, :]
    lanes = lax.broadcasted_iota(jnp.int32, row.shape, 1)
    for p in range(3):
        rms_out[p] = jnp.sum(jnp.where(lanes == p, row, 0.0))
    for c in copies:
        c.wait()


def body(tokens, grad_out, w_gate, w_up, w_down):
    c = tokens.shape[1]
    h = w_gate.shape[0]
    vmem = pl.BlockSpec(memory_space=pltpu.VMEM)
    hbm = pl.BlockSpec(memory_space=pl.ANY)
    dma = pltpu.SemaphoreType.DMA
    grad_in, wgrads, rms = pl.pallas_call(
        kernel,
        out_shape=(
            pltpu.VMEM(tokens.shape, BF16),
            pltpu.VMEM((3, h, c), F32),
            pltpu.VMEM((8, 128), F32),
        ),
        in_specs=[vmem, vmem, hbm, hbm, hbm],
        out_specs=(vmem, vmem, vmem),
        scratch_shapes=[
            pltpu.VMEM((2, STEPS, 2, Y, 8, c), BF16),
            pltpu.VMEM((3, 256, c), BF16),
            pltpu.VMEM((128, c), BF16),
            pltpu.VMEM((128, c), BF16),
            pltpu.VMEM((STEPS, X, 16, 896), F32),
            pltpu.VMEM((STEPS, 3, 16, 896), BF16),
            pltpu.VMEM((STEPS, 3, 16, 896), BF16),
            pltpu.VMEM((STEPS, X, 16, 896), BF16),
            pltpu.VMEM((2, STEPS, 64, c), BF16),
            pltpu.VMEM((2, STEPS, 64, c), BF16),
            pltpu.VMEM((STEPS, X, 16, 896), BF16),
            pltpu.VMEM((STEPS, 2, Y, 8, c), F32),
            pltpu.VMEM((STEPS, 3, 2, 8, c), BF16),
            pltpu.VMEM((STEPS, 3, 2, 8, c), BF16),
            pltpu.VMEM((STEPS, 2, 8, c), BF16),
            pltpu.VMEM((Z - 1, 8, c), BF16),
            pltpu.VMEM((8, c), F32),
            pltpu.VMEM((X * Y * 2, 8, 128), F32),
            pltpu.VMEM((Z, 8, 128), F32),
            pltpu.VMEM((2, 8, 128), F32),
            dma((2, 3)), dma((2, 3)), dma((6,)), dma((6,)), dma((6,)),
            dma((2, STEPS, 4)), dma((2, STEPS, 4)),
            dma((STEPS,)), dma((STEPS,)), dma((STEPS,)), dma((STEPS,)),
            dma((STEPS,)), dma((STEPS,)), dma((STEPS, 2)), dma,
            dma((2, STEPS)), dma((2, STEPS)), dma((STEPS,)), dma((STEPS,)),
            dma((2,)), dma((2,)),
        ],
        compiler_params=pltpu.CompilerParams(
            collective_id=0, has_side_effects=True, vmem_limit_bytes=64_700_000
        ),
    )(tokens, grad_out, w_gate, w_up, w_down)
    wgrad = jax.ShapeDtypeStruct((h, c), F32)
    return pl.pallas_call(
        finish,
        out_shape=(
            jax.ShapeDtypeStruct(tokens.shape, BF16),
            wgrad,
            wgrad,
            wgrad,
            jax.ShapeDtypeStruct((3,), F32),
        ),
        in_specs=[hbm, hbm, vmem],
        out_specs=(hbm, hbm, hbm, hbm, pl.BlockSpec(memory_space=pltpu.SMEM)),
        scratch_shapes=[dma((4,))],
        compiler_params=pltpu.CompilerParams(vmem_limit_bytes=1024 * 1024),
    )(grad_in, wgrads, rms)


def solution(mesh):
    torus = Mesh(
        mesh.devices.reshape(mesh.shape["row"], mesh.shape["col"], 4, 2),
        ("row", "col", "depth_0", "depth_1"),
    )
    placed = P(ROW_DEPTH, "col")
    return jax.shard_map(
        body,
        mesh=torus,
        in_specs=(placed,) * 5,
        out_specs=(placed, placed, placed, placed, P()),
        check_vma=False,
    )
```

```python
import functools

import jax
import jax.numpy as jnp
from jax import lax
from jax.experimental import pallas as pl
from jax.experimental.pallas import tpu as pltpu
from jax.sharding import Mesh
from jax.sharding import PartitionSpec as P

D = 4608
FF = 18432
ROW_DEPTH = ("row", "depth_0", "depth_1")
Z, X, Y = 16, 4, 4
STEPS = Z // 2
ZL = 384
CHUNKS = 4
F32 = jnp.float32
BF16 = jnp.bfloat16
MESH = pl.DeviceIdType.MESH

tanh_scale = 0.7978845608028654
cubic_coeff = 0.044715


def gelu_parts(pre_act):
    inner_arg = tanh_scale * (pre_act + cubic_coeff * pre_act * pre_act * pre_act)
    tanh_value = jnp.tanh(inner_arg)
    gelu_value = 0.5 * pre_act * (1.0 + tanh_value)
    gelu_slope = 0.5 * (1.0 + tanh_value) + 0.5 * pre_act * (
        1.0 - tanh_value * tanh_value
    ) * tanh_scale * (1.0 + 3.0 * cubic_coeff * pre_act * pre_act)
    return (gelu_value, gelu_slope)


def geglu_backward(gate_pre, up_pre, grad_hidden):
    gelu_value, gelu_slope = gelu_parts(gate_pre)
    return (
        gelu_value * up_pre,
        grad_hidden * up_pre * gelu_slope,
        grad_hidden * gelu_value,
    )


def nt(a, b):
    return lax.dot_general(a, b, (((1,), (1,)), ((), ())), preferred_element_type=F32)


def nn(a, b):
    return lax.dot_general(a, b, (((1,), (0,)), ((), ())), preferred_element_type=F32)


def tn(a, b):
    return lax.dot_general(a, b, (((0,), (0,)), ((), ())), preferred_element_type=F32)


def kernel(
    x_ref, dy_ref, wg_ref, wu_ref, wd_ref,
    gi_out, w_out, rms_out,
    blk, wm, wlx, wld, pf, sx, rx, g, xs, ga, gb, gi, sy, ry, sz, rz, acc,
    plane, line, sb, wacc,
    feed, ysend, yrecv, wlocal, wsend, wrecv, send, frecv, urecv, vrecv,
    xgsend, xrecv, grecv, ryrecv, rzsend, rzrecv,
    mxrecv, mgsend, mgrecv, nsend, nrecv, wsem,
):
    z = lax.axis_index("row")
    x = lax.axis_index("col")
    y = lax.axis_index("depth_0")
    k = lax.axis_index("depth_1")

    def zdev(o):
        return {"row": lax.rem(z + o, Z)}

    def xdev(o):
        return {"col": lax.rem(x + o, X)}

    def ydev(o):
        return {"depth_0": lax.rem(y + o, Y)}

    mate = {"depth_1": 1 - k}

    def rcopy(src, dst, s, r, dev):
        return pltpu.make_async_remote_copy(
            src_ref=src, dst_ref=dst, send_sem=s, recv_sem=r, device_id=dev, device_id_type=MESH
        )

    def wait_bytes(ref, sem, name="w"):
        with jax.named_scope("wait_" + name):
            pltpu.make_async_copy(ref, ref, sem).wait()

    barrier = pltpu.get_barrier_semaphore()
    near = [zdev(1), zdev(Z - 1), mate]
    near += [xdev(o) for o in range(1, X)] + [ydev(o) for o in range(1, Y)]
    for dev in near:
        pl.semaphore_signal(barrier, inc=1, device_id=dev, device_id_type=MESH)

    weights = (wg_ref, wu_ref, wd_ref)

    def tail_of(p):
        return (wlx, 0) if p == 0 else (wlx, 32) if p == 1 else (wld, 64)

    local = []
    for p in range(3):
        tail, at = tail_of(p)
        local.append(
            pltpu.make_async_copy(weights[p].at[0:128], wm.at[p, 0:128], wlocal.at[p])
        )
        local.append(
            pltpu.make_async_copy(
                weights[p].at[128:144], tail.at[at : at + 16], wlocal.at[p]
            )
        )
    feeds = [
        pltpu.make_async_copy(src, blk.at[0, 0, xd, y], feed)
        for xd, src in ((0, x_ref), (1, dy_ref))
    ]
    for c in feeds + local:
        c.start()
    wlx[64:128, :] = jnp.zeros((64, wlx.shape[1]), BF16)
    wld[0:64, :] = jnp.zeros((64, wld.shape[1]), BF16)
    wld[96:128, :] = jnp.zeros((32, wld.shape[1]), BF16)
    wait_bytes(blk.at[0, 0, 0, 0:2], feed)

    with jax.named_scope("barrier"):
        pl.semaphore_wait(barrier, len(near))

    def chunk(direction, slot, q):
        at = ZL * max(q - 1, 0)
        return blk.at[direction, slot, min(q, 1), :, :, at : at + ZL]

    def unit(direction, slot):
        return blk.at[direction, slot, 0, y, :, ZL:]

    def along(direction):
        return zdev(1) if direction == 0 else zdev(Z - 1)

    def ring(direction, src_dir, src_slot, dst_dir, dst_slot, q, t):
        return rcopy(
            chunk(src_dir, src_slot, q),
            chunk(dst_dir, dst_slot, q),
            send.at[src_slot],
            frecv.at[direction, lax.rem(t, 3), q],
            along(direction),
        )

    def unit_ring(direction, src_dir, src_slot, dst_dir, dst_slot, t):
        return rcopy(
            unit(src_dir, src_slot),
            unit(dst_dir, dst_slot),
            send.at[src_slot],
            urecv.at[direction, lax.rem(t, 3)],
            along(direction),
        )

    unit_ring(0, 0, 0, 0, 1, 1).start()
    unit_ring(1, 0, 0, 1, 1, 1).start()
    for o in (2, 1, 3):
        for xd in range(2):
            own_unit = blk.at[0, 0, xd, y]
            rcopy(own_unit, own_unit, ysend, yrecv.at[xd], ydev(o)).start()

    def enter(q):
        ring(0, 0, 0, 0, 1, q, 1).start()
        ring(1, 0, 0, 1, 1, q, 1).start()

    for p in range(3):
        tail, at = tail_of(p)
        rcopy(
            weights[p].at[0:128], wm.at[p, 128:256], wsend.at[p], wrecv.at[p], mate
        ).start()
        rcopy(
            weights[p].at[128:144], tail.at[at + 16 : at + 32], wsend.at[p], wrecv.at[p], mate
        ).start()

    wait_bytes(blk.at[0, 0, 0, 0:3], yrecv.at[0], "y")
    enter(0)
    wait_bytes(blk.at[0, 0, 1, 0:3], yrecv.at[1], "y")
    for q in range(1, CHUNKS):
        enter(q)

    for p in range(3):
        wait_bytes(wm.at[0, 0:144], wlocal.at[p], "w")
        wait_bytes(wm.at[0, 0:144], wrecv.at[p], "w")

    def got(direction, slot, q, t, way):
        wait_bytes(chunk(direction, slot, q), frecv.at[way, lax.rem(t, 3), q], "ring")

    def last_way(q):
        return 0 if q < 2 else 1

    def poll(t, q):
        @pl.when(t < STEPS)
        def _():
            for direction in range(2):
                got(direction, t, q, t, direction)

                @pl.when(t < STEPS - 1)
                def _():
                    ring(direction, direction, t, direction, t + 1, q, t + 1).start()

                if direction == last_way(q):

                    @pl.when(t == STEPS - 1)
                    def _():
                        ring(direction, direction, t, 1, 0, q, t + 1).start()

        @pl.when(t == STEPS)
        def _():
            got(1, 0, q, t, last_way(q))

    def spread(direction, slot, t):
        for o in (2, 1, 3):
            rcopy(
                unit(direction, slot),
                unit(direction, slot),
                send.at[t - 1],
                vrecv.at[lax.rem(t, 4)],
                ydev(o),
            ).start()

    def poll_unit(t):
        @pl.when(t < STEPS)
        def _():
            for direction in range(2):
                wait_bytes(unit(direction, t), urecv.at[direction, lax.rem(t, 3)], "unit")

                @pl.when(t < STEPS - 1)
                def _():
                    unit_ring(direction, direction, t, direction, t + 1, t + 1).start()

                if direction == 0:

                    @pl.when(t == STEPS - 1)
                    def _():
                        unit_ring(0, 0, t, 1, 0, t + 1).start()

                spread(direction, t, t)

        @pl.when(t == STEPS)
        def _():
            wait_bytes(unit(1, 0), urecv.at[0, lax.rem(t, 3)], "unit")
            spread(1, 0, t)

    def wait_spread(t):
        @pl.when(t < STEPS)
        def _():
            wait_bytes(blk.at[:, t, 0, 0:3, :, ZL:], vrecv.at[lax.rem(t, 4)], "spread")

        @pl.when(t == STEPS)
        def _():
            wait_bytes(blk.at[1, 0, 0, 0:3, :, ZL:], vrecv.at[lax.rem(t, 4)], "spread")

    poll_unit(1)

    def rows_of(t, xd):
        slot = lax.rem(t, STEPS)
        return blk[:, pl.ds(slot, 1), xd].astype(F32).reshape(64, -1).astype(BF16)

    def put(i, value, at):
        pf[pl.ds(i, 1), :, :, at : at + value.shape[1]] = value.reshape(1, X, 16, -1)

    def to_mate(src, dst, s, r):
        rcopy(src, dst, s, r, mate).start()

    lane = lax.broadcasted_iota(jnp.int32, (16, 128), 1)

    def stage_b(i):
        wait_bytes(rx.at[i], xrecv.at[i], "rx")
        total = pf[i, x]
        for o in range(3):
            total = total + rx[i, o].astype(F32)
        hid, gg, gu = geglu_backward(total[:, 0:256], total[:, 256:512], total[:, 512:768])
        left = total[:, 768:896]
        hid_l, gg_l, gu_l = geglu_backward(
            left, pltpu.roll(left, 96, 1), pltpu.roll(left, 64, 1)
        )
        packed = jnp.where(
            lane < 32,
            gg_l,
            jnp.where(
                lane < 64,
                pltpu.roll(gu_l, 32, 1),
                jnp.where(lane < 96, pltpu.roll(hid_l, 64, 1), 0.0),
            ),
        )
        g[i, x, :, 0:256] = gg.astype(BF16)
        g[i, x, :, 256:512] = gu.astype(BF16)
        g[i, x, :, 512:768] = hid.astype(BF16)
        g[i, x, :, 768:896] = packed.astype(BF16)
        for o in (2, 1, 3):
            rcopy(g.at[i, x], g.at[i, x], xgsend.at[i], grecv.at[i], xdev(o)).start()

    def stage_c(i):
        wait_bytes(g.at[i, 0:3], grecv.at[i], "g")
        gv = g[i].reshape(64, 896)
        tail = gv[:, 768:896]
        for p in range(3):
            gb[i, :, 128 * p : 128 * p + 128] = gv[:, 256 * p + 128 : 256 * p + 256]
        gb[i, :, 384:512] = pltpu.roll(tail.astype(F32), 112, 1).astype(BF16)
        to_mate(gb.at[i], ga.at[i, 1], mgsend, mgrecv.at[i])
        for p in range(3):
            ga[i, 0, :, 128 * p : 128 * p + 128] = gv[:, 256 * p : 256 * p + 128]
        ga[i, 0, :, 384:512] = tail
        part = (
            nn(gv[:, 0:256], wm[0]) + nn(gv[:, 256:512], wm[1]) + nn(gv[:, 768:896], wlx[...])
        )
        gi[pl.ds(i, 1)] = part.reshape(1, 2, Y, 8, -1)
        for o in (2, 1, 3):
            j = lax.rem(y + o, Y)
            sy[i, o - 1] = gi[i, :, j].astype(BF16)
            rcopy(
                sy.at[i, o - 1], ry.at[i, o - 1], send.at[i], ryrecv.at[i], ydev(o)
            ).start()

    def stage_d(i, last=False):
        wait_bytes(ry.at[i], ryrecv.at[i], "ry")
        total = gi[i, :, y]
        for o in range(3):
            total = total + ry[i, o].astype(F32)
        sz[i] = total.astype(BF16)
        t = i + 1

        @pl.when(t < STEPS)
        def _():
            rcopy(
                sz.at[i, 0], rz.at[t - 1], send.at[i], rzrecv, zdev(Z - t)
            ).start()

        @pl.when(t == STEPS)
        def _():
            acc[...] = total[0]

        rcopy(
            sz.at[i, 1],
            rz.at[STEPS - 2 + t],
            rzsend if last else send.at[i],
            rzrecv,
            zdev(t),
        ).start()

    def scoped(f, name):
        def inner(*args):
            with jax.named_scope("stage_" + name):
                f(*args)
        return inner

    stage_b, stage_c, stage_d = scoped(stage_b, "b"), scoped(stage_c, "c"), scoped(stage_d, "d")

    def wgrad(first, n, fresh, p):
        with jax.named_scope("wgrad"):
            if p == 0:
                for j in range(n):
                    wait_bytes(ga.at[first + j, 1], mgrecv.at[first + j], "mg")
                    wait_bytes(xs.at[:, first + j, 1], mxrecv.at[first + j], "mx")
            gv = ga[pl.ds(first, n)].reshape(128 * n, 512)
            right = xs[p // 2, pl.ds(first, n)].reshape(128 * n, -1)
            news = [(p, 0, tn(gv[:, 128 * p : 128 * p + 128], right))]
            if p != 1:
                tail = tn(gv[:, 384:512], right)
                if p == 0:
                    news += [(0, 128, tail[0:16]), (1, 128, tail[32:48])]
                else:
                    news += [(2, 128, tail[64:80])]
            squares = {}
            for q, at, new in news:
                rows = new.shape[0]
                if not fresh:
                    new = wacc[q, at : at + rows] + new
                wacc[q, at : at + rows] = new
                squares[q, at] = jnp.sum((new * new).reshape(rows // 8, 8, -1), axis=0)
            return squares

    def step(t, carry):
        i = t - 1
        poll(t, 0)
        poll(t, 1)
        pl.when(t < STEPS)(lambda: poll_unit(t + 1))
        poll(t, 2)
        pl.when(t >= 3)(lambda: stage_b(t - 3))
        with jax.named_scope("a_x"):
            wait_spread(t)
            xv = rows_of(t, 0)
            xs[0, pl.ds(i, 1), 0] = xv[None]
            put(i, nt(xv, wm[0]), 0)
            put(i, nt(xv, wm[1]), 256)
            left = nt(xv, wlx[...])
        poll(t, 3)
        pl.when(t >= 5)(lambda: stage_c(t - 5))
        with jax.named_scope("a_d"):
            dv = rows_of(t, 1)
            xs[1, pl.ds(i, 1), 0] = dv[None]
            put(i, nt(dv, wm[2]), 512)
            put(i, left + nt(dv, wld[...]), 768)
            for o in (2, 1, 3):
                j = lax.rem(x + o, X)
                sx[i, o - 1] = pf[i, j].astype(BF16)
                rcopy(
                    sx.at[i, o - 1], rx.at[i, o - 1], xgsend.at[i], xrecv.at[i], xdev(o)
                ).start()
            for xd in range(2):
                to_mate(
                    xs.at[xd, i, 0], xs.at[xd, i, 1], send.at[i], mxrecv.at[i]
                )
        pl.when(t >= 7)(lambda: stage_d(t - 7))
        return carry

    lax.fori_loop(1, STEPS + 1, step, 0)

    def more(first, n, fresh=False):
        for p in range(3):
            wgrad(first, n, fresh, p)

    stage_c(4)
    stage_d(2)
    stage_b(6)
    stage_c(5)
    stage_b(7)
    more(0, 4, True)
    stage_d(3)
    stage_c(6)
    stage_d(4)
    more(4, 2)
    stage_d(5)
    stage_c(7)
    squares = {}
    for p in range(3):
        squares.update(wgrad(6, 2, False, p))
    value = jnp.zeros((8, 128), F32)
    for p in range(3):
        value = jnp.where(lane[0:8] == p, jnp.sum(squares[p, 0] + squares[p, 128]), value)

    here = (x * Y + y) * 2 + k
    sb[0] = value
    plane[here] = value
    for dx in (2, 1, 3, 0):
        for dy in (2, 1, 3, 0):
            for dk in (1, 0):
                if dx or dy or dk:
                    rcopy(
                        sb.at[0],
                        plane.at[here],
                        nsend.at[0],
                        nrecv.at[0],
                        {
                            "col": lax.rem(x + dx, X),
                            "depth_0": lax.rem(y + dy, Y),
                            "depth_1": lax.rem(k + dk, 2),
                        },
                    ).start()
    wcopy = pltpu.make_async_copy(wacc, w_out, wsem)
    wcopy.start()
    stage_d(6)
    stage_d(7, True)
    others = X * Y * 2 - 1
    wait_bytes(plane.at[0:others], nrecv.at[0], "plane")
    value = jnp.sum(plane[...], axis=0)
    sb[1] = value
    line[z] = value
    for o in range(Z // 2, 0, -1):
        for d in sorted({o, Z - o}):
            rcopy(sb.at[1], line.at[z], nsend.at[1], nrecv.at[1], zdev(d)).start()

    wait_bytes(rz, rzrecv, "rz")
    total = acc[...]
    for j in range(Z - 1):
        total = total + rz[j].astype(F32)
    gi_out[...] = total.astype(BF16)

    wait_bytes(wacc.at[0, 0:24], ysend)
    for p in range(3):
        wait_bytes(wm.at[0, 0:144], wsend.at[p])
    for i in range(STEPS):
        wait_bytes(wacc.at[0:2, 0:80] if i < STEPS - 1 else wacc.at[0, 0:120], send.at[i])
        wait_bytes(pf.at[0, 0:3], xgsend.at[i])
    wait_bytes(ga.at[:, 0], mgsend)
    wait_bytes(sz.at[0, 1], rzsend)
    wait_bytes(plane.at[0:others], nsend.at[0])
    wcopy.wait()

    wait_bytes(line.at[0 : Z - 1], nrecv.at[1], "line")
    rms_out[...] = jnp.sqrt(jnp.sum(line[...], axis=0) / F32(D * FF))
    wait_bytes(line.at[0 : Z - 1], nsend.at[1])


def finish(gi_ref, w_ref, rms_ref, gi_out, gw_out, uw_out, dw_out, rms_out, sems):
    copies = [
        pltpu.make_async_copy(w_ref.at[p], out, sems.at[p])
        for p, out in enumerate((gw_out, uw_out, dw_out))
    ]
    copies.append(pltpu.make_async_copy(gi_ref, gi_out, sems.at[3]))
    for c in copies:
        c.start()
    row = rms_ref[0:1, :]
    lanes = lax.broadcasted_iota(jnp.int32, row.shape, 1)
    for p in range(3):
        rms_out[p] = jnp.sum(jnp.where(lanes == p, row, 0.0))
    for c in copies:
        c.wait()


def body(tokens, grad_out, w_gate, w_up, w_down):
    c = tokens.shape[1]
    h = w_gate.shape[0]
    vmem = pl.BlockSpec(memory_space=pltpu.VMEM)
    hbm = pl.BlockSpec(memory_space=pl.ANY)
    dma = pltpu.SemaphoreType.DMA
    grad_in, wgrads, rms = pl.pallas_call(
        kernel,
        out_shape=(
            pltpu.VMEM(tokens.shape, BF16),
            pltpu.VMEM((3, h, c), F32),
            pltpu.VMEM((8, 128), F32),
        ),
        in_specs=[hbm] * 5,
        out_specs=(vmem, hbm, vmem),
        scratch_shapes=[
            pltpu.VMEM((2, STEPS, 2, Y, 8, c), BF16),
            pltpu.VMEM((3, 256, c), BF16),
            pltpu.VMEM((128, c), BF16),
            pltpu.VMEM((128, c), BF16),
            pltpu.VMEM((STEPS, X, 16, 896), F32),
            pltpu.VMEM((STEPS, 3, 16, 896), BF16),
            pltpu.VMEM((STEPS, 3, 16, 896), BF16),
            pltpu.VMEM((STEPS, X, 16, 896), BF16),
            pltpu.VMEM((2, STEPS, 2, 64, c), BF16),
            pltpu.VMEM((STEPS, 2, 64, 512), BF16),
            pltpu.VMEM((STEPS, 64, 512), BF16),
            pltpu.VMEM((STEPS, 2, Y, 8, c), F32),
            pltpu.VMEM((STEPS, 3, 2, 8, c), BF16),
            pltpu.VMEM((STEPS, 3, 2, 8, c), BF16),
            pltpu.VMEM((STEPS, 2, 8, c), BF16),
            pltpu.VMEM((Z - 1, 8, c), BF16),
            pltpu.VMEM((8, c), F32),
            pltpu.VMEM((X * Y * 2, 8, 128), F32),
            pltpu.VMEM((Z, 8, 128), F32),
            pltpu.VMEM((2, 8, 128), F32),
            pltpu.VMEM((3, h, c), F32),
            dma, dma, dma((2,)), dma((3,)), dma((3,)), dma((3,)), dma((STEPS,)),
            dma((2, 3, CHUNKS)), dma((2, 3)), dma((4,)),
            dma((STEPS,)), dma((STEPS,)), dma((STEPS,)), dma((STEPS,)), dma, dma,
            dma((STEPS,)), dma, dma((STEPS,)), dma((2,)), dma((2,)), dma,
        ],
        compiler_params=pltpu.CompilerParams(
            collective_id=0, has_side_effects=True, vmem_limit_bytes=64_700_000
        ),
    )(tokens, grad_out, w_gate, w_up, w_down)
    wgrad = jax.ShapeDtypeStruct((h, c), F32)
    return pl.pallas_call(
        finish,
        out_shape=(
            jax.ShapeDtypeStruct(tokens.shape, BF16),
            wgrad,
            wgrad,
            wgrad,
            jax.ShapeDtypeStruct((3,), F32),
        ),
        in_specs=[hbm, hbm, vmem],
        out_specs=(hbm, hbm, hbm, hbm, pl.BlockSpec(memory_space=pltpu.SMEM)),
        scratch_shapes=[dma((4,))],
        compiler_params=pltpu.CompilerParams(vmem_limit_bytes=1024 * 1024),
    )(grad_in, wgrads, rms)


def solution(mesh):
    torus = Mesh(
        mesh.devices.reshape(mesh.shape["row"], mesh.shape["col"], 4, 2),
        ("row", "col", "depth_0", "depth_1"),
    )
    placed = P(ROW_DEPTH, "col")
    return jax.shard_map(
        body,
        mesh=torus,
        in_specs=(placed,) * 5,
        out_specs=(placed, placed, placed, placed, P()),
        check_vma=False,
    )
```

```python
import functools

import jax
import jax.numpy as jnp
from jax import lax
from jax.experimental import pallas as pl
from jax.experimental.pallas import tpu as pltpu
from jax.sharding import Mesh
from jax.sharding import PartitionSpec as P

D = 4608
FF = 18432
ROW_DEPTH = ("row", "depth_0", "depth_1")
Z, X, Y = 16, 4, 4
STEPS = Z // 2
ZL = 384
CHUNKS = 4
F32 = jnp.float32
BF16 = jnp.bfloat16
MESH = pl.DeviceIdType.MESH

tanh_scale = 0.7978845608028654
cubic_coeff = 0.044715


def gelu_parts(pre_act):
    inner_arg = tanh_scale * (pre_act + cubic_coeff * pre_act * pre_act * pre_act)
    tanh_value = jnp.tanh(inner_arg)
    gelu_value = 0.5 * pre_act * (1.0 + tanh_value)
    gelu_slope = 0.5 * (1.0 + tanh_value) + 0.5 * pre_act * (
        1.0 - tanh_value * tanh_value
    ) * tanh_scale * (1.0 + 3.0 * cubic_coeff * pre_act * pre_act)
    return (gelu_value, gelu_slope)


def geglu_backward(gate_pre, up_pre, grad_hidden):
    gelu_value, gelu_slope = gelu_parts(gate_pre)
    return (
        gelu_value * up_pre,
        grad_hidden * up_pre * gelu_slope,
        grad_hidden * gelu_value,
    )


def nt(a, b):
    return lax.dot_general(a, b, (((1,), (1,)), ((), ())), preferred_element_type=F32)


def nn(a, b):
    return lax.dot_general(a, b, (((1,), (0,)), ((), ())), preferred_element_type=F32)


def tn(a, b):
    return lax.dot_general(a, b, (((0,), (0,)), ((), ())), preferred_element_type=F32)


def kernel(
    x_ref, dy_ref, wg_ref, wu_ref, wd_ref,
    gi_out, w_out, rms_out,
    blk, wm, wlx, wld, pf, sx, rx, g, xs, ga, gb, gi, sy, ry, sz, rz, acc,
    plane, line, sb, wacc, own,
    feed, hrecv, ysend, yrecv, wlocal, wsend, wrecv, send, frecv, urecv, vrecv,
    xgsend, xrecv, grecv, ryrecv, rzsend, rzrecv,
    precv, mgsend, mgrecv, nsend, nrecv, wsem,
):
    z = lax.axis_index("row")
    x = lax.axis_index("col")
    y = lax.axis_index("depth_0")
    k = lax.axis_index("depth_1")

    def zdev(o):
        return {"row": lax.rem(z + o, Z)}

    def xdev(o):
        return {"col": lax.rem(x + o, X)}

    def ydev(o):
        return {"depth_0": lax.rem(y + o, Y)}

    mate = {"depth_1": 1 - k}

    def rcopy(src, dst, s, r, dev):
        return pltpu.make_async_remote_copy(
            src_ref=src, dst_ref=dst, send_sem=s, recv_sem=r, device_id=dev, device_id_type=MESH
        )

    def wait_bytes(ref, sem, name="w"):
        with jax.named_scope("wait_" + name):
            pltpu.make_async_copy(ref, ref, sem).wait()

    barrier = pltpu.get_barrier_semaphore()
    near = [zdev(1), zdev(Z - 1), mate]
    near += [xdev(o) for o in range(1, X)] + [ydev(o) for o in range(1, Y)]
    near += [{**ydev(o), **mate} for o in range(1, Y)]
    for dev in near:
        pl.semaphore_signal(barrier, inc=1, device_id=dev, device_id_type=MESH)

    weights = (wg_ref, wu_ref, wd_ref)

    def tail_of(p):
        return (wlx, 0) if p == 0 else (wlx, 32) if p == 1 else (wld, 64)

    local = []
    for p in range(3):
        tail, at = tail_of(p)
        local.append(
            pltpu.make_async_copy(weights[p].at[0:128], wm.at[p, 0:128], wlocal.at[p])
        )
        local.append(
            pltpu.make_async_copy(
                weights[p].at[128:144], tail.at[at : at + 16], wlocal.at[p]
            )
        )
    feeds = [
        pltpu.make_async_copy(src, own.at[xd], feed.at[0])
        for xd, src in ((0, x_ref), (1, dy_ref))
    ]
    for c in feeds + local:
        c.start()

    @pl.when(k == 1)
    def _():
        for xd, src in ((0, x_ref), (1, dy_ref)):
            pltpu.make_async_copy(src, blk.at[0, 0, 1, xd, y], feed.at[1]).start()

    wlx[64:128, :] = jnp.zeros((64, wlx.shape[1]), BF16)
    wld[0:64, :] = jnp.zeros((64, wld.shape[1]), BF16)
    wld[96:128, :] = jnp.zeros((32, wld.shape[1]), BF16)
    wait_bytes(own, feed.at[0])

    @pl.when(k == 1)
    def _():
        wait_bytes(own, feed.at[1])


    with jax.named_scope("barrier"):
        pl.semaphore_wait(barrier, len(near))

    def chunk(direction, slot, q):
        at = ZL * max(q - 1, 0)
        return blk.at[direction, slot, :, min(q, 1), :, :, at : at + ZL]

    def unit(direction, slot):
        return blk.at[direction, slot, :, 0, y, :, ZL:]

    def along(direction):
        return zdev(1) if direction == 0 else zdev(Z - 1)

    def ring(direction, src_dir, src_slot, dst_dir, dst_slot, q, t):
        return rcopy(
            chunk(src_dir, src_slot, q),
            chunk(dst_dir, dst_slot, q),
            send.at[src_slot],
            frecv.at[direction, lax.rem(t, 3), q],
            along(direction),
        )

    def unit_ring(direction, src_dir, src_slot, dst_dir, dst_slot, t):
        return rcopy(
            unit(src_dir, src_slot),
            unit(dst_dir, dst_slot),
            send.at[src_slot],
            urecv.at[direction, lax.rem(t, 3)],
            along(direction),
        )

    def to_ring(o, xd, r):
        rcopy(
            own.at[xd],
            blk.at[0, 0, k, xd, y],
            ysend,
            r,
            {"depth_0": lax.rem(y + o, Y), "depth_1": 1},
        ).start()

    @pl.when(k == 0)
    def _():
        for xd in range(2):
            to_ring(0, xd, hrecv)

    for o in (2, 1, 3):
        for xd in range(2):
            to_ring(o, xd, yrecv.at[xd])

    def enter(q):
        ring(0, 0, 0, 0, 1, q, 1).start()
        ring(1, 0, 0, 1, 1, q, 1).start()

    for p in range(3):
        tail, at = tail_of(p)
        rcopy(
            weights[p].at[0:128], wm.at[p, 128:256], wsend.at[p], wrecv.at[p], mate
        ).start()
        rcopy(
            weights[p].at[128:144], tail.at[at + 16 : at + 32], wsend.at[p], wrecv.at[p], mate
        ).start()

    def got(direction, slot, q, t, way):
        wait_bytes(chunk(direction, slot, q), frecv.at[way, lax.rem(t, 3), q], "ring")

    def last_way(q):
        return 0 if q < 2 else 1

    def poll(t, q):
        @pl.when(t < STEPS)
        def _():
            for direction in range(2):
                got(direction, t, q, t, direction)

                @pl.when(t < STEPS - 1)
                def _():
                    ring(direction, direction, t, direction, t + 1, q, t + 1).start()

                if direction == last_way(q):

                    @pl.when(t == STEPS - 1)
                    def _():
                        ring(direction, direction, t, 1, 0, q, t + 1).start()

        @pl.when(t == STEPS)
        def _():
            got(1, 0, q, t, last_way(q))

    def spread(direction, slot, t):
        for o in (2, 1, 3):
            rcopy(
                unit(direction, slot),
                unit(direction, slot),
                send.at[t - 1],
                vrecv.at[lax.rem(t, 4)],
                ydev(o),
            ).start()

    def poll_unit(t):
        @pl.when(t < STEPS)
        def _():
            for direction in range(2):
                wait_bytes(unit(direction, t), urecv.at[direction, lax.rem(t, 3)], "unit")

                @pl.when(t < STEPS - 1)
                def _():
                    unit_ring(direction, direction, t, direction, t + 1, t + 1).start()

                if direction == 0:

                    @pl.when(t == STEPS - 1)
                    def _():
                        unit_ring(0, 0, t, 1, 0, t + 1).start()

                spread(direction, t, t)

        @pl.when(t == STEPS)
        def _():
            wait_bytes(unit(1, 0), urecv.at[0, lax.rem(t, 3)], "unit")
            spread(1, 0, t)

    def wait_spread(t):
        @pl.when(t < STEPS)
        def _():
            wait_bytes(blk.at[:, t, :, 0, 0:3, :, ZL:], vrecv.at[lax.rem(t, 4)], "spread")

        @pl.when(t == STEPS)
        def _():
            wait_bytes(blk.at[1, 0, :, 0, 0:3, :, ZL:], vrecv.at[lax.rem(t, 4)], "spread")

    @pl.when(k == 1)
    def _():
        wait_bytes(own, hrecv)
        unit_ring(0, 0, 0, 0, 1, 1).start()
        unit_ring(1, 0, 0, 1, 1, 1).start()
        wait_bytes(blk.at[0, 0, :, 0, 0:3], yrecv.at[0], "y")
        enter(0)
        poll_unit(1)
        wait_bytes(blk.at[0, 0, :, 1, 0:3], yrecv.at[1], "y")
        for q in range(1, CHUNKS):
            enter(q)

    for p in range(3):
        wait_bytes(wm.at[0, 0:144], wlocal.at[p], "w")
        wait_bytes(wm.at[0, 0:144], wrecv.at[p], "w")

    def rows_of(t, core, xd):
        slot = lax.rem(t, STEPS)
        return blk[:, pl.ds(slot, 1), pl.ds(core, 1), xd].astype(F32).reshape(64, -1).astype(BF16)

    def part_of(t, part):
        slot = lax.rem(t, STEPS)
        return blk.at[:, slot, 1] if part == 2 else blk.at[:, slot, 0, part]

    def push(t, part):
        ref = part_of(t, part)
        rcopy(ref, ref, send.at[t - 1], precv.at[part, t - 1], {"depth_1": 0}).start()

    def pushed(t, part):
        wait_bytes(part_of(t, part), precv.at[part, t - 1], "push")

    def stage_m(t):
        pl.when(k == 0)(lambda: pushed(t, 2))
        for xd in range(2):
            xs[xd, pl.ds(t - 1, 1), 1] = rows_of(t, 1 - k, xd)[None]

    def put(i, value, at):
        pf[pl.ds(i, 1), :, :, at : at + value.shape[1]] = value.reshape(1, X, 16, -1)

    def to_mate(src, dst, s, r):
        rcopy(src, dst, s, r, mate).start()

    lane = lax.broadcasted_iota(jnp.int32, (16, 128), 1)

    def stage_b(i):
        wait_bytes(rx.at[i], xrecv.at[i], "rx")
        total = pf[i, x]
        for o in range(3):
            total = total + rx[i, o].astype(F32)
        hid, gg, gu = geglu_backward(total[:, 0:256], total[:, 256:512], total[:, 512:768])
        left = total[:, 768:896]
        hid_l, gg_l, gu_l = geglu_backward(
            left, pltpu.roll(left, 96, 1), pltpu.roll(left, 64, 1)
        )
        packed = jnp.where(
            lane < 32,
            gg_l,
            jnp.where(
                lane < 64,
                pltpu.roll(gu_l, 32, 1),
                jnp.where(lane < 96, pltpu.roll(hid_l, 64, 1), 0.0),
            ),
        )
        g[i, x, :, 0:256] = gg.astype(BF16)
        g[i, x, :, 256:512] = gu.astype(BF16)
        g[i, x, :, 512:768] = hid.astype(BF16)
        g[i, x, :, 768:896] = packed.astype(BF16)
        for o in (2, 1, 3):
            rcopy(g.at[i, x], g.at[i, x], xgsend.at[i], grecv.at[i], xdev(o)).start()

    def stage_c(i):
        wait_bytes(g.at[i, 0:3], grecv.at[i], "g")
        gv = g[i].reshape(64, 896)
        tail = gv[:, 768:896]
        for p in range(3):
            gb[i, :, 128 * p : 128 * p + 128] = gv[:, 256 * p + 128 : 256 * p + 256]
        gb[i, :, 384:512] = pltpu.roll(tail.astype(F32), 112, 1).astype(BF16)
        to_mate(gb.at[i], ga.at[i, 1], mgsend, mgrecv.at[i])
        for p in range(3):
            ga[i, 0, :, 128 * p : 128 * p + 128] = gv[:, 256 * p : 256 * p + 128]
        ga[i, 0, :, 384:512] = tail
        part = (
            nn(gv[:, 0:256], wm[0]) + nn(gv[:, 256:512], wm[1]) + nn(gv[:, 768:896], wlx[...])
        )
        gi[pl.ds(i, 1)] = part.reshape(1, 2, Y, 8, -1)
        for o in (2, 1, 3):
            j = lax.rem(y + o, Y)
            sy[i, o - 1] = gi[i, :, j].astype(BF16)
            rcopy(
                sy.at[i, o - 1], ry.at[i, o - 1], send.at[i], ryrecv.at[i], ydev(o)
            ).start()

    def stage_d(i, last=False):
        wait_bytes(ry.at[i], ryrecv.at[i], "ry")
        total = gi[i, :, y]
        for o in range(3):
            total = total + ry[i, o].astype(F32)
        sz[i] = total.astype(BF16)
        t = i + 1

        @pl.when(t < STEPS)
        def _():
            rcopy(
                sz.at[i, 0], rz.at[t - 1], send.at[i], rzrecv, zdev(Z - t)
            ).start()

        @pl.when(t == STEPS)
        def _():
            acc[...] = total[0]

        rcopy(
            sz.at[i, 1],
            rz.at[STEPS - 2 + t],
            rzsend if last else send.at[i],
            rzrecv,
            zdev(t),
        ).start()

    def scoped(f, name):
        def inner(*args):
            with jax.named_scope("stage_" + name):
                f(*args)
        return inner

    stage_b, stage_c, stage_d = scoped(stage_b, "b"), scoped(stage_c, "c"), scoped(stage_d, "d")

    def wgrad(first, n, fresh, p):
        with jax.named_scope("wgrad"):
            if p == 0:
                for j in range(n):
                    wait_bytes(ga.at[first + j, 1], mgrecv.at[first + j], "mg")
            gv = ga[pl.ds(first, n)].reshape(128 * n, 512)
            right = xs[p // 2, pl.ds(first, n)].reshape(128 * n, -1)
            news = [(p, 0, tn(gv[:, 128 * p : 128 * p + 128], right))]
            if p != 1:
                tail = tn(gv[:, 384:512], right)
                if p == 0:
                    news += [(0, 128, tail[0:16]), (1, 128, tail[32:48])]
                else:
                    news += [(2, 128, tail[64:80])]
            squares = {}
            for q, at, new in news:
                rows = new.shape[0]
                if not fresh:
                    new = wacc[q, at : at + rows] + new
                wacc[q, at : at + rows] = new
                squares[q, at] = jnp.sum((new * new).reshape(rows // 8, 8, -1), axis=0)
            return squares

    def step(t, carry):
        i = t - 1

        @pl.when(k == 1)
        def _():
            poll(t, 0)
            poll(t, 1)
            pl.when(t < STEPS)(lambda: poll_unit(t + 1))
            poll(t, 2)

        pl.when(t >= 3)(lambda: stage_b(t - 3))

        @pl.when(k == 1)
        def _():
            wait_spread(t)
            push(t, 0)

        pl.when(k == 0)(lambda: pushed(t, 0))
        with jax.named_scope("a_x"):
            xv = rows_of(t, k, 0)
            xs[0, pl.ds(i, 1), 0] = xv[None]
            put(i, nt(xv, wm[0]), 0)
            put(i, nt(xv, wm[1]), 256)
            left = nt(xv, wlx[...])

        @pl.when(k == 1)
        def _():
            poll(t, 3)
            push(t, 1)
            push(t, 2)

        pl.when(t >= 5)(lambda: stage_c(t - 5))
        pl.when(k == 0)(lambda: pushed(t, 1))
        with jax.named_scope("a_d"):
            dv = rows_of(t, k, 1)
            xs[1, pl.ds(i, 1), 0] = dv[None]
            put(i, nt(dv, wm[2]), 512)
            put(i, left + nt(dv, wld[...]), 768)
            for o in (2, 1, 3):
                j = lax.rem(x + o, X)
                sx[i, o - 1] = pf[i, j].astype(BF16)
                rcopy(
                    sx.at[i, o - 1], rx.at[i, o - 1], xgsend.at[i], xrecv.at[i], xdev(o)
                ).start()
        pl.when(t >= 2)(lambda: stage_m(t - 1))
        pl.when(t >= 7)(lambda: stage_d(t - 7))
        return carry

    lax.fori_loop(1, STEPS + 1, step, 0)

    def more(first, n, fresh=False):
        for p in range(3):
            wgrad(first, n, fresh, p)

    stage_c(4)
    stage_m(STEPS)
    stage_d(2)
    stage_b(6)
    stage_c(5)
    stage_b(7)
    more(0, 4, True)
    stage_d(3)
    stage_c(6)
    stage_d(4)
    more(4, 2)
    stage_d(5)
    stage_c(7)
    squares = {}
    for p in range(3):
        squares.update(wgrad(6, 2, False, p))
    value = jnp.zeros((8, 128), F32)
    for p in range(3):
        value = jnp.where(lane[0:8] == p, jnp.sum(squares[p, 0] + squares[p, 128]), value)

    here = (x * Y + y) * 2 + k
    sb[0] = value
    plane[here] = value
    for dx in (2, 1, 3, 0):
        for dy in (2, 1, 3, 0):
            for dk in (1, 0):
                if dx or dy or dk:
                    rcopy(
                        sb.at[0],
                        plane.at[here],
                        nsend.at[0],
                        nrecv.at[0],
                        {
                            "col": lax.rem(x + dx, X),
                            "depth_0": lax.rem(y + dy, Y),
                            "depth_1": lax.rem(k + dk, 2),
                        },
                    ).start()
    wcopy = pltpu.make_async_copy(wacc, w_out, wsem)
    wcopy.start()
    stage_d(6)
    stage_d(7, True)
    others = X * Y * 2 - 1
    wait_bytes(plane.at[0:others], nrecv.at[0], "plane")
    value = jnp.sum(plane[...], axis=0)
    sb[1] = value
    line[z] = value
    for o in range(Z // 2, 0, -1):
        for d in sorted({o, Z - o}):
            rcopy(sb.at[1], line.at[z], nsend.at[1], nrecv.at[1], zdev(d)).start()

    wait_bytes(rz, rzrecv, "rz")
    total = acc[...]
    for j in range(Z - 1):
        total = total + rz[j].astype(F32)
    gi_out[...] = total.astype(BF16)

    for p in range(3):
        wait_bytes(wm.at[0, 0:144], wsend.at[p])

    @pl.when(k == 1)
    def _():
        wait_bytes(wacc.at[0, 0:24], ysend)
        for i in range(STEPS):
            wait_bytes(wacc.at[0:2, 0:144] if i < STEPS - 1 else wacc.at[0:3, 0:72], send.at[i])

    @pl.when(k == 0)
    def _():
        wait_bytes(wacc.at[0, 0:32], ysend)
        for i in range(STEPS):
            wait_bytes(wacc.at[0, 0:32] if i < STEPS - 1 else wacc.at[0, 0:24], send.at[i])

    for i in range(STEPS):
        wait_bytes(pf.at[0, 0:3], xgsend.at[i])
    wait_bytes(ga.at[:, 0], mgsend)
    wait_bytes(sz.at[0, 1], rzsend)
    wait_bytes(plane.at[0:others], nsend.at[0])
    wcopy.wait()

    wait_bytes(line.at[0 : Z - 1], nrecv.at[1], "line")
    rms_out[...] = jnp.sqrt(jnp.sum(line[...], axis=0) / F32(D * FF))
    wait_bytes(line.at[0 : Z - 1], nsend.at[1])


def finish(gi_ref, w_ref, rms_ref, gi_out, gw_out, uw_out, dw_out, rms_out, sems):
    copies = [
        pltpu.make_async_copy(w_ref.at[p], out, sems.at[p])
        for p, out in enumerate((gw_out, uw_out, dw_out))
    ]
    copies.append(pltpu.make_async_copy(gi_ref, gi_out, sems.at[3]))
    for c in copies:
        c.start()
    row = rms_ref[0:1, :]
    lanes = lax.broadcasted_iota(jnp.int32, row.shape, 1)
    for p in range(3):
        rms_out[p] = jnp.sum(jnp.where(lanes == p, row, 0.0))
    for c in copies:
        c.wait()


def body(tokens, grad_out, w_gate, w_up, w_down):
    c = tokens.shape[1]
    h = w_gate.shape[0]
    vmem = pl.BlockSpec(memory_space=pltpu.VMEM)
    hbm = pl.BlockSpec(memory_space=pl.ANY)
    dma = pltpu.SemaphoreType.DMA
    grad_in, wgrads, rms = pl.pallas_call(
        kernel,
        out_shape=(
            pltpu.VMEM(tokens.shape, BF16),
            pltpu.VMEM((3, h, c), F32),
            pltpu.VMEM((8, 128), F32),
        ),
        in_specs=[hbm] * 5,
        out_specs=(vmem, hbm, vmem),
        scratch_shapes=[
            pltpu.VMEM((2, STEPS, 2, 2, Y, 8, c), BF16),
            pltpu.VMEM((3, 256, c), BF16),
            pltpu.VMEM((128, c), BF16),
            pltpu.VMEM((128, c), BF16),
            pltpu.VMEM((STEPS, X, 16, 896), F32),
            pltpu.VMEM((STEPS, 3, 16, 896), BF16),
            pltpu.VMEM((STEPS, 3, 16, 896), BF16),
            pltpu.VMEM((STEPS, X, 16, 896), BF16),
            pltpu.VMEM((2, STEPS, 2, 64, c), BF16),
            pltpu.VMEM((STEPS, 2, 64, 512), BF16),
            pltpu.VMEM((STEPS, 64, 512), BF16),
            pltpu.VMEM((STEPS, 2, Y, 8, c), F32),
            pltpu.VMEM((STEPS, 3, 2, 8, c), BF16),
            pltpu.VMEM((STEPS, 3, 2, 8, c), BF16),
            pltpu.VMEM((STEPS, 2, 8, c), BF16),
            pltpu.VMEM((Z - 1, 8, c), BF16),
            pltpu.VMEM((8, c), F32),
            pltpu.VMEM((X * Y * 2, 8, 128), F32),
            pltpu.VMEM((Z, 8, 128), F32),
            pltpu.VMEM((2, 8, 128), F32),
            pltpu.VMEM((3, h, c), F32),
            pltpu.VMEM((2, 8, c), BF16),
            dma((2,)), dma, dma, dma((2,)), dma((3,)), dma((3,)), dma((3,)), dma((STEPS,)),
            dma((2, 3, CHUNKS)), dma((2, 3)), dma((4,)),
            dma((STEPS,)), dma((STEPS,)), dma((STEPS,)), dma((STEPS,)), dma, dma,
            dma((3, STEPS)), dma, dma((STEPS,)), dma((2,)), dma((2,)), dma,
        ],
        compiler_params=pltpu.CompilerParams(
            collective_id=0, has_side_effects=True, vmem_limit_bytes=64_700_000
        ),
    )(tokens, grad_out, w_gate, w_up, w_down)
    wgrad = jax.ShapeDtypeStruct((h, c), F32)
    return pl.pallas_call(
        finish,
        out_shape=(
            jax.ShapeDtypeStruct(tokens.shape, BF16),
            wgrad,
            wgrad,
            wgrad,
            jax.ShapeDtypeStruct((3,), F32),
        ),
        in_specs=[hbm, hbm, vmem],
        out_specs=(hbm, hbm, hbm, hbm, pl.BlockSpec(memory_space=pltpu.SMEM)),
        scratch_shapes=[dma((4,))],
        compiler_params=pltpu.CompilerParams(vmem_limit_bytes=1024 * 1024),
    )(grad_in, wgrads, rms)


def solution(mesh):
    torus = Mesh(
        mesh.devices.reshape(mesh.shape["row"], mesh.shape["col"], 4, 2),
        ("row", "col", "depth_0", "depth_1"),
    )
    placed = P(ROW_DEPTH, "col")
    return jax.shard_map(
        body,
        mesh=torus,
        in_specs=(placed,) * 5,
        out_specs=(placed, placed, placed, placed, P()),
        check_vma=False,
    )
```

```python
import functools

import jax
import jax.numpy as jnp
from jax import lax
from jax.experimental import pallas as pl
from jax.experimental.pallas import tpu as pltpu
from jax.sharding import Mesh
from jax.sharding import PartitionSpec as P

D = 4608
FF = 18432
ROW_DEPTH = ("row", "depth_0", "depth_1")
Z, X, Y = 16, 4, 4
STEPS = Z // 2
ZL = 384
CHUNKS = 4
F32 = jnp.float32
BF16 = jnp.bfloat16
MESH = pl.DeviceIdType.MESH

tanh_scale = 0.7978845608028654
cubic_coeff = 0.044715


def gelu_parts(pre_act):
    inner_arg = tanh_scale * (pre_act + cubic_coeff * pre_act * pre_act * pre_act)
    tanh_value = jnp.tanh(inner_arg)
    gelu_value = 0.5 * pre_act * (1.0 + tanh_value)
    gelu_slope = 0.5 * (1.0 + tanh_value) + 0.5 * pre_act * (
        1.0 - tanh_value * tanh_value
    ) * tanh_scale * (1.0 + 3.0 * cubic_coeff * pre_act * pre_act)
    return (gelu_value, gelu_slope)


def geglu_backward(gate_pre, up_pre, grad_hidden):
    gelu_value, gelu_slope = gelu_parts(gate_pre)
    return (
        gelu_value * up_pre,
        grad_hidden * up_pre * gelu_slope,
        grad_hidden * gelu_value,
    )


def nt(a, b):
    return lax.dot_general(a, b, (((1,), (1,)), ((), ())), preferred_element_type=F32)


def nn(a, b):
    return lax.dot_general(a, b, (((1,), (0,)), ((), ())), preferred_element_type=F32)


def tn(a, b):
    return lax.dot_general(a, b, (((0,), (0,)), ((), ())), preferred_element_type=F32)


def kernel(
    x_ref, dy_ref, wg_ref, wu_ref, wd_ref,
    gi_out, w_out, rms_out,
    blk, wm, wlx, wld, pf, sx, rx, g, xs, ga, gb, gi, sy, ry, sz, rz, acc,
    plane, line, sb, wacc, own,
    feed, hrecv, ysend, yrecv, wlocal, wsend, wrecv, send, frecv, urecv, vrecv,
    xgsend, xrecv, grecv, ryrecv, rzsend, rzrecv,
    precv, mgsend, mgrecv, nsend, nrecv, wsem,
):
    z = lax.axis_index("row")
    x = lax.axis_index("col")
    y = lax.axis_index("depth_0")
    k = lax.axis_index("depth_1")

    def zdev(o):
        return {"row": lax.rem(z + o, Z)}

    def xdev(o):
        return {"col": lax.rem(x + o, X)}

    def ydev(o):
        return {"depth_0": lax.rem(y + o, Y)}

    mate = {"depth_1": 1 - k}

    def rcopy(src, dst, s, r, dev):
        return pltpu.make_async_remote_copy(
            src_ref=src, dst_ref=dst, send_sem=s, recv_sem=r, device_id=dev, device_id_type=MESH
        )

    def wait_bytes(ref, sem, name="w"):
        with jax.named_scope("wait_" + name):
            pltpu.make_async_copy(ref, ref, sem).wait()

    barrier = pltpu.get_barrier_semaphore()
    near = [zdev(1), zdev(Z - 1), mate]
    near += [xdev(o) for o in range(1, X)] + [ydev(o) for o in range(1, Y)]
    near += [{**ydev(o), **mate} for o in range(1, Y)]
    for dev in near:
        pl.semaphore_signal(barrier, inc=1, device_id=dev, device_id_type=MESH)

    weights = (wg_ref, wu_ref, wd_ref)

    def tail_of(p):
        return (wlx, 0) if p == 0 else (wlx, 32) if p == 1 else (wld, 64)

    local = []
    for p in range(3):
        tail, at = tail_of(p)
        local.append(
            pltpu.make_async_copy(weights[p].at[0:128], wm.at[p, 0:128], wlocal.at[p])
        )
        local.append(
            pltpu.make_async_copy(
                weights[p].at[128:144], tail.at[at : at + 16], wlocal.at[p]
            )
        )
    feeds = [
        pltpu.make_async_copy(src, own.at[xd], feed.at[0])
        for xd, src in ((0, x_ref), (1, dy_ref))
    ]
    for c in feeds + local:
        c.start()

    @pl.when(k == 1)
    def _():
        for xd, src in ((0, x_ref), (1, dy_ref)):
            pltpu.make_async_copy(src, blk.at[0, 0, 1, xd, y], feed.at[1]).start()

    wlx[64:128, :] = jnp.zeros((64, wlx.shape[1]), BF16)
    wld[0:64, :] = jnp.zeros((64, wld.shape[1]), BF16)
    wld[96:128, :] = jnp.zeros((32, wld.shape[1]), BF16)
    wait_bytes(own, feed.at[0])

    @pl.when(k == 1)
    def _():
        wait_bytes(own, feed.at[1])


    with jax.named_scope("barrier"):
        pl.semaphore_wait(barrier, len(near))

    def chunk(direction, slot, q):
        at = ZL * max(q - 1, 0)
        return blk.at[direction, slot, :, min(q, 1), :, :, at : at + ZL]

    def unit(direction, slot):
        return blk.at[direction, slot, :, 0, y, :, ZL:]

    def along(direction):
        return zdev(1) if direction == 0 else zdev(Z - 1)

    def ring(direction, src_dir, src_slot, dst_dir, dst_slot, q, t):
        return rcopy(
            chunk(src_dir, src_slot, q),
            chunk(dst_dir, dst_slot, q),
            send.at[src_slot],
            frecv.at[direction, lax.rem(t, 3), q],
            along(direction),
        )

    def unit_ring(direction, src_dir, src_slot, dst_dir, dst_slot, t):
        return rcopy(
            unit(src_dir, src_slot),
            unit(dst_dir, dst_slot),
            send.at[src_slot],
            urecv.at[direction, lax.rem(t, 3)],
            along(direction),
        )

    def to_ring(o, xd, r):
        rcopy(
            own.at[xd],
            blk.at[0, 0, k, xd, y],
            ysend,
            r,
            {"depth_0": lax.rem(y + o, Y), "depth_1": 1},
        ).start()

    @pl.when(k == 0)
    def _():
        for xd in range(2):
            to_ring(0, xd, hrecv)

    for xd in range(2):
        for o in (2, 1, 3):
            to_ring(o, xd, yrecv.at[xd])

    def enter(q):
        ring(0, 0, 0, 0, 1, q, 1).start()
        ring(1, 0, 0, 1, 1, q, 1).start()

    for p in range(3):
        tail, at = tail_of(p)
        rcopy(
            weights[p].at[0:128], wm.at[p, 128:256], wsend.at[p], wrecv.at[p], mate
        ).start()
        rcopy(
            weights[p].at[128:144], tail.at[at + 16 : at + 32], wsend.at[p], wrecv.at[p], mate
        ).start()

    def got(direction, slot, q, t, way):
        wait_bytes(chunk(direction, slot, q), frecv.at[way, lax.rem(t, 3), q], "ring")

    def last_way(q):
        return 0 if q < 2 else 1

    def poll(t, q):
        @pl.when(t < STEPS)
        def _():
            for direction in range(2):
                got(direction, t, q, t, direction)

                @pl.when(t < STEPS - 1)
                def _():
                    ring(direction, direction, t, direction, t + 1, q, t + 1).start()

                if direction == last_way(q):

                    @pl.when(t == STEPS - 1)
                    def _():
                        ring(direction, direction, t, 1, 0, q, t + 1).start()

        @pl.when(t == STEPS)
        def _():
            got(1, 0, q, t, last_way(q))

    def spread(direction, slot, t):
        for o in (2, 1, 3):
            rcopy(
                unit(direction, slot),
                unit(direction, slot),
                send.at[t - 1],
                vrecv.at[lax.rem(t, 4)],
                ydev(o),
            ).start()

    def poll_unit(t):
        @pl.when(t < STEPS)
        def _():
            for direction in range(2):
                wait_bytes(unit(direction, t), urecv.at[direction, lax.rem(t, 3)], "unit")

                @pl.when(t < STEPS - 1)
                def _():
                    unit_ring(direction, direction, t, direction, t + 1, t + 1).start()

                if direction == 0:

                    @pl.when(t == STEPS - 1)
                    def _():
                        unit_ring(0, 0, t, 1, 0, t + 1).start()

                spread(direction, t, t)

        @pl.when(t == STEPS)
        def _():
            wait_bytes(unit(1, 0), urecv.at[0, lax.rem(t, 3)], "unit")
            spread(1, 0, t)

    def wait_spread(t):
        @pl.when(t < STEPS)
        def _():
            wait_bytes(blk.at[:, t, :, 0, 0:3, :, ZL:], vrecv.at[lax.rem(t, 4)], "spread")

        @pl.when(t == STEPS)
        def _():
            wait_bytes(blk.at[1, 0, :, 0, 0:3, :, ZL:], vrecv.at[lax.rem(t, 4)], "spread")

    @pl.when(k == 1)
    def _():
        wait_bytes(own, hrecv)
        unit_ring(0, 0, 0, 0, 1, 1).start()
        unit_ring(1, 0, 0, 1, 1, 1).start()
        wait_bytes(blk.at[0, 0, :, 0, 0:3], yrecv.at[0], "y")
        enter(0)
        poll_unit(1)
        wait_bytes(blk.at[0, 0, :, 1, 0:3], yrecv.at[1], "y")
        for q in range(1, CHUNKS):
            enter(q)

    for p in range(3):
        wait_bytes(wm.at[0, 0:144], wlocal.at[p], "w")
        wait_bytes(wm.at[0, 0:144], wrecv.at[p], "w")

    def rows_of(t, core, xd):
        slot = lax.rem(t, STEPS)
        return blk[:, pl.ds(slot, 1), pl.ds(core, 1), xd].astype(F32).reshape(64, -1).astype(BF16)

    def part_of(t, part):
        slot = lax.rem(t, STEPS)
        return blk.at[:, slot, 1] if part == 2 else blk.at[:, slot, 0, part]

    def push(t, part):
        ref = part_of(t, part)
        rcopy(ref, ref, send.at[t - 1], precv.at[part, t - 1], {"depth_1": 0}).start()

    def pushed(t, part):
        wait_bytes(part_of(t, part), precv.at[part, t - 1], "push")

    def stage_m(t):
        pl.when(k == 0)(lambda: pushed(t, 2))
        for xd in range(2):
            xs[xd, pl.ds(t - 1, 1), 1] = rows_of(t, 1 - k, xd)[None]

    def put(i, value, at):
        pf[pl.ds(i, 1), :, :, at : at + value.shape[1]] = value.reshape(1, X, 16, -1)

    def to_mate(src, dst, s, r):
        rcopy(src, dst, s, r, mate).start()

    lane = lax.broadcasted_iota(jnp.int32, (16, 128), 1)

    def stage_b(i):
        wait_bytes(rx.at[i], xrecv.at[i], "rx")
        total = pf[i, x]
        for o in range(3):
            total = total + rx[i, o].astype(F32)
        hid, gg, gu = geglu_backward(total[:, 0:256], total[:, 256:512], total[:, 512:768])
        left = total[:, 768:896]
        hid_l, gg_l, gu_l = geglu_backward(
            left, pltpu.roll(left, 96, 1), pltpu.roll(left, 64, 1)
        )
        packed = jnp.where(
            lane < 32,
            gg_l,
            jnp.where(
                lane < 64,
                pltpu.roll(gu_l, 32, 1),
                jnp.where(lane < 96, pltpu.roll(hid_l, 64, 1), 0.0),
            ),
        )
        g[i, x, :, 0:256] = gg.astype(BF16)
        g[i, x, :, 256:512] = gu.astype(BF16)
        g[i, x, :, 512:768] = hid.astype(BF16)
        g[i, x, :, 768:896] = packed.astype(BF16)
        for o in (2, 1, 3):
            rcopy(g.at[i, x], g.at[i, x], xgsend.at[i], grecv.at[i], xdev(o)).start()

    def stage_c(i):
        wait_bytes(g.at[i, 0:3], grecv.at[i], "g")
        gv = g[i].reshape(64, 896)
        tail = gv[:, 768:896]
        for p in range(3):
            gb[i, :, 128 * p : 128 * p + 128] = gv[:, 256 * p + 128 : 256 * p + 256]
        gb[i, :, 384:512] = pltpu.roll(tail.astype(F32), 112, 1).astype(BF16)
        to_mate(gb.at[i], ga.at[i, 1], mgsend, mgrecv.at[i])
        for p in range(3):
            ga[i, 0, :, 128 * p : 128 * p + 128] = gv[:, 256 * p : 256 * p + 128]
        ga[i, 0, :, 384:512] = tail
        part = (
            nn(gv[:, 0:256], wm[0]) + nn(gv[:, 256:512], wm[1]) + nn(gv[:, 768:896], wlx[...])
        )
        gi[pl.ds(i, 1)] = part.reshape(1, 2, Y, 8, -1)
        for o in (2, 1, 3):
            j = lax.rem(y + o, Y)
            sy[i, o - 1] = gi[i, :, j].astype(BF16)
            rcopy(
                sy.at[i, o - 1], ry.at[i, o - 1], send.at[i], ryrecv.at[i], ydev(o)
            ).start()

    def stage_d(i, last=False):
        wait_bytes(ry.at[i], ryrecv.at[i], "ry")
        total = gi[i, :, y]
        for o in range(3):
            total = total + ry[i, o].astype(F32)
        sz[i] = total.astype(BF16)
        t = i + 1

        @pl.when(t < STEPS)
        def _():
            rcopy(
                sz.at[i, 0], rz.at[t - 1], send.at[i], rzrecv, zdev(Z - t)
            ).start()

        @pl.when(t == STEPS)
        def _():
            acc[...] = total[0]

        rcopy(
            sz.at[i, 1],
            rz.at[STEPS - 2 + t],
            rzsend if last else send.at[i],
            rzrecv,
            zdev(t),
        ).start()

    def scoped(f, name):
        def inner(*args):
            with jax.named_scope("stage_" + name):
                f(*args)
        return inner

    stage_b, stage_c, stage_d = scoped(stage_b, "b"), scoped(stage_c, "c"), scoped(stage_d, "d")

    def wgrad(first, n, fresh, p):
        with jax.named_scope("wgrad"):
            if p == 0:
                for j in range(n):
                    wait_bytes(ga.at[first + j, 1], mgrecv.at[first + j], "mg")
            gv = ga[pl.ds(first, n)].reshape(128 * n, 512)
            right = xs[p // 2, pl.ds(first, n)].reshape(128 * n, -1)
            news = [(p, 0, tn(gv[:, 128 * p : 128 * p + 128], right))]
            if p != 1:
                tail = tn(gv[:, 384:512], right)
                if p == 0:
                    news += [(0, 128, tail[0:16]), (1, 128, tail[32:48])]
                else:
                    news += [(2, 128, tail[64:80])]
            squares = {}
            for q, at, new in news:
                rows = new.shape[0]
                if not fresh:
                    new = wacc[q, at : at + rows] + new
                wacc[q, at : at + rows] = new
                squares[q, at] = jnp.sum((new * new).reshape(rows // 8, 8, -1), axis=0)
            return squares

    def step(t, carry):
        i = t - 1

        @pl.when(k == 1)
        def _():
            poll(t, 0)
            poll(t, 1)
            pl.when(t < STEPS)(lambda: poll_unit(t + 1))
            poll(t, 2)

        pl.when(t >= 3)(lambda: stage_b(t - 3))

        @pl.when(k == 1)
        def _():
            wait_spread(t)
            push(t, 0)

        pl.when(k == 0)(lambda: pushed(t, 0))
        with jax.named_scope("a_x"):
            xv = rows_of(t, k, 0)
            xs[0, pl.ds(i, 1), 0] = xv[None]
            put(i, nt(xv, wm[0]), 0)
            put(i, nt(xv, wm[1]), 256)
            left = nt(xv, wlx[...])

        @pl.when(k == 1)
        def _():
            poll(t, 3)
            push(t, 1)
            push(t, 2)

        pl.when(t >= 5)(lambda: stage_c(t - 5))
        pl.when(k == 0)(lambda: pushed(t, 1))
        with jax.named_scope("a_d"):
            dv = rows_of(t, k, 1)
            xs[1, pl.ds(i, 1), 0] = dv[None]
            put(i, nt(dv, wm[2]), 512)
            put(i, left + nt(dv, wld[...]), 768)
            for o in (2, 1, 3):
                j = lax.rem(x + o, X)
                sx[i, o - 1] = pf[i, j].astype(BF16)
                rcopy(
                    sx.at[i, o - 1], rx.at[i, o - 1], xgsend.at[i], xrecv.at[i], xdev(o)
                ).start()
        pl.when(t >= 2)(lambda: stage_m(t - 1))
        pl.when(t >= 7)(lambda: stage_d(t - 7))
        return carry

    lax.fori_loop(1, STEPS + 1, step, 0)

    def more(first, n, fresh=False):
        for p in range(3):
            wgrad(first, n, fresh, p)

    stage_c(4)
    stage_m(STEPS)
    stage_d(2)
    stage_b(6)
    stage_c(5)
    stage_b(7)
    more(0, 4, True)
    stage_d(3)
    stage_c(6)
    stage_d(4)
    more(4, 2)
    stage_d(5)
    stage_c(7)
    squares = wgrad(6, 2, False, 0)
    stage_d(6)
    for p in (1, 2):
        squares.update(wgrad(6, 2, False, p))
    value = jnp.zeros((8, 128), F32)
    for p in range(3):
        value = jnp.where(lane[0:8] == p, jnp.sum(squares[p, 0] + squares[p, 128]), value)

    here = (x * Y + y) * 2 + k
    sb[0] = value
    plane[here] = value
    for dx in (2, 1, 3, 0):
        for dy in (2, 1, 3, 0):
            for dk in (1, 0):
                if dx or dy or dk:
                    rcopy(
                        sb.at[0],
                        plane.at[here],
                        nsend.at[0],
                        nrecv.at[0],
                        {
                            "col": lax.rem(x + dx, X),
                            "depth_0": lax.rem(y + dy, Y),
                            "depth_1": lax.rem(k + dk, 2),
                        },
                    ).start()
    wcopy = pltpu.make_async_copy(wacc, w_out, wsem)
    wcopy.start()
    stage_d(7, True)
    others = X * Y * 2 - 1
    wait_bytes(plane.at[0:others], nrecv.at[0], "plane")
    value = jnp.sum(plane[...], axis=0)
    sb[1] = value
    line[z] = value
    for o in range(Z // 2, 0, -1):
        for d in sorted({o, Z - o}):
            rcopy(sb.at[1], line.at[z], nsend.at[1], nrecv.at[1], zdev(d)).start()

    wait_bytes(rz, rzrecv, "rz")
    total = acc[...]
    for j in range(Z - 1):
        total = total + rz[j].astype(F32)
    gi_out[...] = total.astype(BF16)

    for p in range(3):
        wait_bytes(wm.at[0, 0:144], wsend.at[p])

    @pl.when(k == 1)
    def _():
        wait_bytes(wacc.at[0, 0:24], ysend)
        for i in range(STEPS):
            wait_bytes(wacc.at[0:2, 0:144] if i < STEPS - 1 else wacc.at[0:3, 0:72], send.at[i])

    @pl.when(k == 0)
    def _():
        wait_bytes(wacc.at[0, 0:32], ysend)
        for i in range(STEPS):
            wait_bytes(wacc.at[0, 0:32] if i < STEPS - 1 else wacc.at[0, 0:24], send.at[i])

    for i in range(STEPS):
        wait_bytes(pf.at[0, 0:3], xgsend.at[i])
    wait_bytes(ga.at[:, 0], mgsend)
    wait_bytes(sz.at[0, 1], rzsend)
    wait_bytes(plane.at[0:others], nsend.at[0])
    wcopy.wait()

    wait_bytes(line.at[0 : Z - 1], nrecv.at[1], "line")
    rms_out[...] = jnp.sqrt(jnp.sum(line[...], axis=0) / F32(D * FF))
    wait_bytes(line.at[0 : Z - 1], nsend.at[1])


def finish(gi_ref, w_ref, rms_ref, gi_out, gw_out, uw_out, dw_out, rms_out, sems):
    copies = [
        pltpu.make_async_copy(w_ref.at[p], out, sems.at[p])
        for p, out in enumerate((gw_out, uw_out, dw_out))
    ]
    copies.append(pltpu.make_async_copy(gi_ref, gi_out, sems.at[3]))
    for c in copies:
        c.start()
    row = rms_ref[0:1, :]
    lanes = lax.broadcasted_iota(jnp.int32, row.shape, 1)
    for p in range(3):
        rms_out[p] = jnp.sum(jnp.where(lanes == p, row, 0.0))
    for c in copies:
        c.wait()


def body(tokens, grad_out, w_gate, w_up, w_down):
    c = tokens.shape[1]
    h = w_gate.shape[0]
    vmem = pl.BlockSpec(memory_space=pltpu.VMEM)
    hbm = pl.BlockSpec(memory_space=pl.ANY)
    dma = pltpu.SemaphoreType.DMA
    grad_in, wgrads, rms = pl.pallas_call(
        kernel,
        out_shape=(
            pltpu.VMEM(tokens.shape, BF16),
            pltpu.VMEM((3, h, c), F32),
            pltpu.VMEM((8, 128), F32),
        ),
        in_specs=[hbm] * 5,
        out_specs=(vmem, hbm, vmem),
        scratch_shapes=[
            pltpu.VMEM((2, STEPS, 2, 2, Y, 8, c), BF16),
            pltpu.VMEM((3, 256, c), BF16),
            pltpu.VMEM((128, c), BF16),
            pltpu.VMEM((128, c), BF16),
            pltpu.VMEM((STEPS, X, 16, 896), F32),
            pltpu.VMEM((STEPS, 3, 16, 896), BF16),
            pltpu.VMEM((STEPS, 3, 16, 896), BF16),
            pltpu.VMEM((STEPS, X, 16, 896), BF16),
            pltpu.VMEM((2, STEPS, 2, 64, c), BF16),
            pltpu.VMEM((STEPS, 2, 64, 512), BF16),
            pltpu.VMEM((STEPS, 64, 512), BF16),
            pltpu.VMEM((STEPS, 2, Y, 8, c), F32),
            pltpu.VMEM((STEPS, 3, 2, 8, c), BF16),
            pltpu.VMEM((STEPS, 3, 2, 8, c), BF16),
            pltpu.VMEM((STEPS, 2, 8, c), BF16),
            pltpu.VMEM((Z - 1, 8, c), BF16),
            pltpu.VMEM((8, c), F32),
            pltpu.VMEM((X * Y * 2, 8, 128), F32),
            pltpu.VMEM((Z, 8, 128), F32),
            pltpu.VMEM((2, 8, 128), F32),
            pltpu.VMEM((3, h, c), F32),
            pltpu.VMEM((2, 8, c), BF16),
            dma((2,)), dma, dma, dma((2,)), dma((3,)), dma((3,)), dma((3,)), dma((STEPS,)),
            dma((2, 3, CHUNKS)), dma((2, 3)), dma((4,)),
            dma((STEPS,)), dma((STEPS,)), dma((STEPS,)), dma((STEPS,)), dma, dma,
            dma((3, STEPS)), dma, dma((STEPS,)), dma((2,)), dma((2,)), dma,
        ],
        compiler_params=pltpu.CompilerParams(
            collective_id=0, has_side_effects=True, vmem_limit_bytes=64_700_000
        ),
    )(tokens, grad_out, w_gate, w_up, w_down)
    wgrad = jax.ShapeDtypeStruct((h, c), F32)
    return pl.pallas_call(
        finish,
        out_shape=(
            jax.ShapeDtypeStruct(tokens.shape, BF16),
            wgrad,
            wgrad,
            wgrad,
            jax.ShapeDtypeStruct((3,), F32),
        ),
        in_specs=[hbm, hbm, vmem],
        out_specs=(hbm, hbm, hbm, hbm, pl.BlockSpec(memory_space=pltpu.SMEM)),
        scratch_shapes=[dma((4,))],
        compiler_params=pltpu.CompilerParams(vmem_limit_bytes=1024 * 1024),
    )(grad_in, wgrads, rms)


def solution(mesh):
    torus = Mesh(
        mesh.devices.reshape(mesh.shape["row"], mesh.shape["col"], 4, 2),
        ("row", "col", "depth_0", "depth_1"),
    )
    placed = P(ROW_DEPTH, "col")
    return jax.shard_map(
        body,
        mesh=torus,
        in_specs=(placed,) * 5,
        out_specs=(placed, placed, placed, placed, P()),
        check_vma=False,
    )
```
